128 devices in a mesh: gx: 16 (over y, x_lo, core), gy: 8 (over z, x_hi).
Axes of the slice: x: 4 (x_hi: 2, x_lo: 2; x = x_hi * 2 + x_lo), y: 4, z: 4, core: 2. Of those that a mesh axis runs over, the one named last changes fastest.
Arguments:
- thinker_normed: bfloat16 [8, 16, 8192], P(None, None, 'gx'), may hold values from -6 to 6
- thinker_resid: bfloat16 [8, 16, 8192], P('gy', None, 'gx'), may hold values from -6 to 6
- gate_weight: bfloat16 [8192, 29568], P('gx', 'gy'), may hold values from -0.0625 to 0.0625
- up_weight: bfloat16 [8192, 29568], P('gx', 'gy'), may hold values from -0.0625 to 0.0625
- down_weight: bfloat16 [29568, 8192], P('gy', 'gx'), may hold values from -0.03125 to 0.03125
- bridge_weight: bfloat16 [8192, 3584], P('gx'), may hold values from -0.0625 to 0.0625
- talker_stream: bfloat16 [8, 3072, 3584], P('gy', 'gx'), may hold values from -6 to 6
- norm_gain: float32 [3584], replicated, may hold values from 0.5 to 2
- w_query: bfloat16 [3584, 1792], P(None, 'gy'), may hold values from -0.09375 to 0.09375
- w_key: bfloat16 [3584, 256], P(None, 'gy'), may hold values from -0.09375 to 0.09375
- w_value: bfloat16 [3584, 256], P(None, 'gy'), may hold values from -0.09375 to 0.09375
- a_query: bfloat16 [3584, 64], replicated, may hold values from -0.09375 to 0.09375
- b_query: bfloat16 [64, 1792], replicated, may hold values from -0.75 to 0.75
- a_value: bfloat16 [3584, 64], replicated, may hold values from -0.09375 to 0.09375
- b_value: bfloat16 [64, 256], replicated, may hold values from -0.75 to 0.75
- text_index: int32 [8, 3072], P('gy', 'gx'), may hold values from 0 to 15
- span_offset: int32 [8], P('gy'), may hold values from 1 to 3071
- out_grad: bfloat16 [8, 3072, 1792], P('gy', 'gx'), may hold values from -6 to 6
Outputs:
- attn_out: bfloat16 [8, 3072, 1792], P('gy', 'gx')
- grad_aq: float32 [3584, 64], replicated
- grad_bq: float32 [64, 1792], replicated
- grad_av: float32 [3584, 64], replicated
- grad_bv: float32 [64, 256], replicated
The draws below stay inside these ranges and needn't reach their ends.
All inputs are finite; a program needn't handle non-finite values.
Results may differ from the reference program's by a relative error of at most 0.035.
Values may be sent and summed in bfloat16 or wider, within the bound.
A program may use at most 192 MiB of HBM per device.

```python
import math
import jax
import jax.numpy as jnp
from jax import lax

DT = 8192
FF = 29568
DM = 3584
HEADS = 14
KVH = 2
HD = 128
RANK = 64
R_SEQ = 16
LEN = 3072
SEQS = 8


def draw_norm_gain(key, part):
    return jax.random.uniform(key, (DM,), jnp.float32, 0.5, 1.5)


def set_ends(result, stream_key, smallest, high):
    longest = result.shape.index(max(result.shape))
    spots = []
    for shift in (0, 1):
        where = [jax.random.randint(jax.random.fold_in(stream_key, axis), (), 0, length) for axis, length in enumerate(result.shape)]
        where[longest] = (where[longest] + shift) % result.shape[longest]
        spots.append(tuple(where))
    return result.at[spots[0]].set(smallest).at[spots[1]].set(high)


def levels(rng, extent, shards, smallest, top_value):
    gain = 1.0
    for dim, parts in shards:
        steps = jax.random.uniform(jax.random.fold_in(jax.random.fold_in(rng, 6), dim), (parts,), jnp.float32, smallest / len(shards), top_value / len(shards))
        gain = gain * jnp.repeat(jnp.exp(steps), extent[dim] // parts).reshape((-1,) + (1,) * (len(extent) - 1 - dim))
    return gain


def noise(rng, dims, deviation, most, split=(), held_as=jnp.bfloat16):
    loudness = levels(rng, dims, split, -0.22, 0.18) if split else 1.0
    drawn = jax.random.normal(rng, dims, jnp.float32) * deviation * loudness
    return jnp.minimum(jnp.maximum(drawn, -most), most).astype(held_as)


def setup_inputs(seed: int = 0) -> dict:
    arg_keys = jax.random.split(jax.random.key(seed), 19)
    thinker_normed = noise(arg_keys[0], (SEQS, R_SEQ, DT), 1.0, 6.0, ((2, 16),))
    thinker_resid = noise(arg_keys[1], (SEQS, R_SEQ, DT), 1.0, 6.0, ((0, 8), (2, 16)))
    gate_weight = noise(arg_keys[2], (DT, FF), DT ** -0.5, 0.0625, ((0, 16), (1, 8)))
    up_weight = noise(arg_keys[3], (DT, FF), DT ** -0.5, 0.0625, ((0, 16), (1, 8)))
    down_weight = noise(arg_keys[4], (FF, DT), FF ** -0.5, 0.03125, ((0, 8), (1, 16)))
    bridge_weight = noise(arg_keys[5], (DT, DM), DT ** -0.5, 0.0625, ((0, 16),))
    talker_stream = noise(arg_keys[6], (SEQS, LEN, DM), 1.0, 6.0, ((0, 8), (1, 16)))
    norm_gain = draw_norm_gain(jax.random.fold_in(arg_keys[18], 71), 0)
    w_query = noise(arg_keys[8], (DM, HEADS * HD), DM ** -0.5, 0.09375, ((1, 8),))
    w_key = noise(arg_keys[9], (DM, KVH * HD), DM ** -0.5, 0.09375, ((1, 8),))
    w_value = noise(arg_keys[10], (DM, KVH * HD), DM ** -0.5, 0.09375, ((1, 8),))
    a_query = noise(arg_keys[11], (DM, RANK), DM ** -0.5, 0.09375)
    b_query = noise(arg_keys[12], (RANK, HEADS * HD), RANK ** -0.5, 0.75)
    a_value = noise(arg_keys[13], (DM, RANK), DM ** -0.5, 0.09375)
    b_value = noise(arg_keys[14], (RANK, KVH * HD), RANK ** -0.5, 0.75)
    text_index = set_ends(jax.random.randint(arg_keys[15], (SEQS, LEN), 0, R_SEQ), jax.random.fold_in(arg_keys[15], 1), 0, R_SEQ - 1).astype(jnp.int32)
    span_offset = set_ends(jax.random.randint(arg_keys[16], (SEQS,), 1, LEN), jax.random.fold_in(arg_keys[16], 1), 1, LEN - 1).astype(jnp.int32)
    out_grad = noise(arg_keys[17], (SEQS, LEN, HEADS * HD), 1.0, 6.0, ((0, 8), (1, 16)))
    return dict(thinker_normed=thinker_normed, thinker_resid=thinker_resid, gate_weight=gate_weight, up_weight=up_weight, down_weight=down_weight, bridge_weight=bridge_weight, talker_stream=talker_stream, norm_gain=norm_gain, w_query=w_query, w_key=w_key, w_value=w_value, a_query=a_query, b_query=b_query, a_value=a_value, b_value=b_value, text_index=text_index, span_offset=span_offset, out_grad=out_grad)


rope_base = 1000000.0
norm_eps = 1e-06

def angle_tables(first_pos, length):
    position = (first_pos + jnp.arange(length, dtype=jnp.int32)).astype(jnp.float32)
    frequency = rope_base ** (-(2.0 * jnp.arange(HD // 2, dtype=jnp.float32)) / HD)
    angles = position[:, None] * frequency[None, :]
    return (jnp.cos(angles), jnp.sin(angles))

def rotate(tensor, cosine, sine_table, signed):
    layout = (cosine.shape[0],) + (1,) * (tensor.ndim - 2) + (cosine.shape[1],)
    cosine = cosine.reshape(layout)
    sine_part = sine_table.reshape(layout) * signed
    half_width = tensor.shape[-1] // 2
    first_half = tensor[..., :half_width]
    second_half = tensor[..., half_width:]
    return jnp.concatenate([first_half * cosine - second_half * sine_part, second_half * cosine + first_half * sine_part], axis=-1)

def reference(thinker_normed, thinker_resid, gate_weight, up_weight, down_weight, bridge_weight, talker_stream, norm_gain, w_query, w_key, w_value, a_query, b_query, a_value, b_value, text_index, span_offset, out_grad):
    normed = thinker_normed.reshape(SEQS * R_SEQ, DT)
    gate_part = jnp.dot(normed, gate_weight, preferred_element_type=jnp.float32)
    up_part = jnp.dot(normed, up_weight, preferred_element_type=jnp.float32)
    hidden = (jax.nn.silu(gate_part) * up_part).astype(jnp.bfloat16)
    thinker_out = (jnp.dot(hidden, down_weight, preferred_element_type=jnp.float32) + thinker_resid.reshape(SEQS * R_SEQ, DT).astype(jnp.float32)).astype(jnp.bfloat16)
    bridge = jnp.dot(thinker_out, bridge_weight, preferred_element_type=jnp.float32).astype(jnp.bfloat16).reshape(SEQS, R_SEQ, DM)
    groups = HEADS // KVH
    scale = 1.0 / math.sqrt(HD)

    def one_sequence(inputs):
        stream, picks, table, offset, cotangent = inputs
        length = stream.shape[0]
        mixed = stream.astype(jnp.float32) + table[picks].astype(jnp.float32)
        normal = (mixed * lax.rsqrt(lax.optimization_barrier(jnp.mean(mixed * mixed, axis=1, keepdims=True)) + norm_eps) * norm_gain).astype(jnp.bfloat16)
        low_query = jnp.dot(normal, a_query, preferred_element_type=jnp.float32).astype(jnp.bfloat16)
        low_value = jnp.dot(normal, a_value, preferred_element_type=jnp.float32).astype(jnp.bfloat16)
        cosine, sine_table = angle_tables(jnp.int32(0), length)
        query_pre = jnp.dot(normal, w_query, preferred_element_type=jnp.float32) + jnp.dot(low_query, b_query, preferred_element_type=jnp.float32)
        query = rotate(query_pre.reshape(length, KVH, groups, HD), cosine, sine_table, 1.0).astype(jnp.bfloat16)
        key_pre = jnp.dot(normal, w_key, preferred_element_type=jnp.float32).reshape(length, KVH, HD)
        key_rows = rotate(key_pre, cosine, sine_table, 1.0).astype(jnp.bfloat16)
        value_pre = jnp.dot(normal, w_value, preferred_element_type=jnp.float32) + jnp.dot(low_value, b_value, preferred_element_type=jnp.float32)
        value_rows = value_pre.astype(jnp.bfloat16).reshape(length, KVH, HD)
        places = jnp.arange(length, dtype=jnp.int32)
        causal = (places[None, :] <= places[:, None]) | (places[None, :] < offset)
        scores = jnp.einsum('tkgd,skd->kgts', query.astype(jnp.float32), key_rows.astype(jnp.float32)) * scale
        scores = jnp.where(causal, scores, -1e+30)
        row_max = lax.optimization_barrier(jnp.max(scores, axis=-1, keepdims=True))
        weights = jnp.exp(scores - row_max)
        probs = (weights / lax.optimization_barrier(jnp.sum(weights, axis=-1, keepdims=True))).astype(jnp.bfloat16)
        attended = jnp.einsum('kgts,skd->tkgd', probs.astype(jnp.float32), value_rows.astype(jnp.float32)).astype(jnp.bfloat16)
        grad_four = cotangent.reshape(length, KVH, groups, HD).astype(jnp.float32)
        inner_prod = lax.optimization_barrier(jnp.sum(grad_four * attended.astype(jnp.float32), axis=-1))
        dprob = jnp.einsum('tkgd,skd->kgts', grad_four, value_rows.astype(jnp.float32))
        dscore = (probs.astype(jnp.float32) * (dprob - jnp.transpose(inner_prod, (1, 2, 0))[..., None])).astype(jnp.bfloat16)
        dquery = jnp.einsum('kgts,skd->tkgd', dscore.astype(jnp.float32), key_rows.astype(jnp.float32)) * scale
        query_grad = rotate(dquery, cosine, sine_table, -1.0).reshape(length, HEADS * HD).astype(jnp.bfloat16)
        dvalue = jnp.einsum('kgts,tkgd->skd', probs.astype(jnp.float32), grad_four)
        value_grad = dvalue.reshape(length, KVH * HD).astype(jnp.bfloat16)
        grad_bq = jnp.dot(low_query.T, query_grad, preferred_element_type=jnp.float32)
        grad_bv = jnp.dot(low_value.T, value_grad, preferred_element_type=jnp.float32)
        dlow_query = jnp.dot(query_grad, b_query.T, preferred_element_type=jnp.float32).astype(jnp.bfloat16)
        dlow_value = jnp.dot(value_grad, b_value.T, preferred_element_type=jnp.float32).astype(jnp.bfloat16)
        grad_aq = jnp.dot(normal.T, dlow_query, preferred_element_type=jnp.float32)
        grad_av = jnp.dot(normal.T, dlow_value, preferred_element_type=jnp.float32)
        return (attended.reshape(length, HEADS * HD), grad_aq, grad_bq, grad_av, grad_bv)
    results = lax.map(one_sequence, (talker_stream, text_index, bridge, span_offset, out_grad))
    return (results[0], lax.optimization_barrier(jnp.sum(results[1], axis=0)), lax.optimization_barrier(jnp.sum(results[2], axis=0)), lax.optimization_barrier(jnp.sum(results[3], axis=0)), lax.optimization_barrier(jnp.sum(results[4], axis=0)))
```

```python
import functools
import math

import jax
import jax.numpy as jnp
from jax import lax
from jax.experimental import pallas as pl
from jax.experimental.pallas import tpu as pltpu
from jax.sharding import PartitionSpec as P

HEADS = 14
KVH = 2
HD = 128
MESH = pl.DeviceIdType.MESH
F32 = jnp.float32
BF16 = jnp.bfloat16

rope_base = 1000000.0
norm_eps = 1e-06


def angle_tables(first_pos, length):
    position = (first_pos + jnp.arange(length, dtype=jnp.int32)).astype(jnp.float32)
    frequency = rope_base ** (-(2.0 * jnp.arange(HD // 2, dtype=jnp.float32)) / HD)
    angles = position[:, None] * frequency[None, :]
    return (jnp.cos(angles), jnp.sin(angles))


def place():
    gx = lax.axis_index("gx")
    gy = lax.axis_index("gy")
    return gx, gy, gx // 2, gx % 2


def greet(peers):
    barrier = pltpu.get_barrier_semaphore()
    for peer in peers:
        pl.semaphore_signal(barrier, inc=1, device_id=peer, device_id_type=MESH)
    pl.semaphore_wait(barrier, len(peers))


def send(src, dst, send_sem, recv_sem, peer):
    copy = pltpu.make_async_remote_copy(
        src_ref=src,
        dst_ref=dst,
        send_sem=send_sem,
        recv_sem=recv_sem,
        device_id=peer,
        device_id_type=MESH,
    )
    copy.start()
    return copy


def dot_nt(a, b):
    return lax.dot_general(a, b, (((1,), (1,)), ((), ())), preferred_element_type=F32)


HALF = 1920
REST = 1776
CHUNK = 640


def thinker_kernel(
    x_ref,
    resid_ref,
    gate_ref,
    up_ref,
    down_ref,
    bridge_ref,
    wq_ref,
    wk_ref,
    wv_ref,
    out_ref,
    all_q,
    all_kv,
    gate_w,
    up_w,
    down_w,
    bridge_w,
    own_q,
    own_kv,
    pair_tx,
    own_half,
    pair_rx,
    chip_tx,
    chip_rx,
    hidden,
    down_own,
    down_tx,
    down_rx,
    bridge_own,
    bridge_rx,
    bridge_tx,
    bridge_peers,
    bridge_half,
    load_sem,
    pair_sem,
    chip_sem,
    hid_sem,
    fwd_sem,
    gy_sem,
    bp_sem,
    bc_sem,
    bf_sem,
    w_sem,
):
    gx, gy, chip, core = place()
    other = 1 - core
    z = gy // 2
    x_hi = gy % 2
    partner = (chip * 2 + other, gy)
    chips = [((chip + k) % 8 * 2 + core, gy) for k in range(1, 8)]
    columns = [(gx, (gy + k) % 8) for k in range(1, 8)]
    cross = ((chip + 1 - 2 * (chip % 2)) * 2 + core, gy + 1 - 2 * x_hi)
    z_up = (gx, (z + 1) % 4 * 2 + x_hi)
    z_down = (gx, (z + 3) % 4 * 2 + x_hi)

    loads = []

    def load(src, dst, i):
        copy = pltpu.make_async_copy(src, dst, load_sem.at[i])
        copy.start()
        loads.append(copy)

    load(wq_ref, own_q, 0)
    load(gate_ref.at[pl.ds(0, HALF)], gate_w.at[0], 1)
    load(gate_ref.at[pl.ds(HALF, REST)], gate_w.at[1, pl.ds(0, REST)], 2)
    load(up_ref.at[pl.ds(0, HALF)], up_w.at[0], 3)
    load(up_ref.at[pl.ds(HALF, REST)], up_w.at[1, pl.ds(0, REST)], 4)
    load(down_ref.at[pl.ds(0, HALF)], down_w.at[0], 5)
    load(down_ref.at[pl.ds(HALF, REST)], down_w.at[1, pl.ds(0, REST)], 6)
    load(bridge_ref, bridge_w, 7)
    load(wk_ref, own_kv.at[0], 8)
    load(wv_ref, own_kv.at[1], 9)
    pad = jnp.zeros((HALF - REST, 512), BF16)
    gate_w[1, REST:] = pad
    up_w[1, REST:] = pad
    down_w[1, REST:] = pad

    greet([partner, cross] + chips + columns)

    for i in (0, 8, 9):
        loads[i].wait()
    own_outs = [
        pltpu.make_async_copy(own_q, all_q.at[gy], load_sem.at[10]),
        pltpu.make_async_copy(own_kv, all_kv.at[:, gy], load_sem.at[11]),
    ]
    for copy in own_outs:
        copy.start()
    cols = pl.ds(pl.multiple_of(core * 1792, 128), 1792)

    def spread(piece, part, i, peer, own=False):
        rows = pl.ds(112 * part, 112) if part is not None else pl.ds(0, 224)
        kinds = pl.ds(part, 1) if part is not None else pl.ds(0, 2)
        q_to, kv_to = all_q.at[piece, rows, cols], all_kv.at[kinds, piece, :, cols]
        q_from = own_q.at[rows, cols] if own else q_to
        kv_from = own_kv.at[kinds, :, cols] if own else kv_to
        return [
            send(q_from, q_to, w_sem.at[0, i], w_sem.at[1, i], peer),
            send(kv_from, kv_to, w_sem.at[2, i], w_sem.at[3, i], peer),
        ]

    def wait_all(copies):
        for copy in copies:
            copy.wait()

    w_sends = [
        spread(gy, None, 0, cross, True),
        spread(gy, None, 1, z_up, True),
        spread(gy, None, 2, z_down, True),
    ]
    forwards = []

    def forward(piece):
        forwards.append(spread(piece, None, 9 + len(forwards), partner))

    for i in range(1, 5):
        loads[i].wait()
    x = x_ref[...]
    for half, is_own in ((other, False), (core, True)):
        for side, weight in ((0, gate_w), (1, up_w)):
            for c in range(HALF // CHUNK):
                part = dot_nt(x, weight[half, c * CHUNK : (c + 1) * CHUNK])
                part = part.reshape(8, 16, CHUNK)
                lo = side * HALF + c * CHUNK
                if is_own:
                    own_half[:, :, lo : lo + CHUNK] = part
                else:
                    pair_tx[:, :, lo : lo + CHUNK] = part.astype(BF16)
        if not is_own:
            pair_copy = send(pair_tx, pair_rx, pair_sem.at[0], pair_sem.at[1], partner)
    pair_copy.wait()

    chip_copies = []
    for k in range(1, 8):
        peer = (chip + k) % 8
        chip_tx[k - 1] = (own_half[peer] + pair_rx[peer].astype(F32)).astype(BF16)
        chip_copies.append(
            send(
                chip_tx.at[k - 1],
                chip_rx.at[k - 1],
                chip_sem.at[0, k - 1],
                chip_sem.at[1, k - 1],
                chips[k - 1],
            )
        )
    total = own_half[chip] + pair_rx[chip].astype(F32)
    for k in range(7):
        chip_copies[k].wait()
        total = total + chip_rx[k].astype(F32)
    gate = total[:, :HALF]
    hidden[core, chip] = (gate / (1.0 + jnp.exp(-gate)) * total[:, HALF:]).astype(BF16)

    hid_copies = [
        send(
            hidden.at[core, chip],
            hidden.at[core, chip],
            hid_sem.at[0, k],
            hid_sem.at[1, k],
            chips[k],
        )
        for k in range(7)
    ]
    hid_fwd = [
        send(
            hidden.at[core, chip],
            hidden.at[core, chip],
            fwd_sem.at[0, 7],
            fwd_sem.at[1, 7],
            partner,
        )
    ]
    for k in range(7):
        hid_copies[k].wait()
        source = (chip + 7 - k) % 8
        hid_fwd.append(
            send(
                hidden.at[core, source],
                hidden.at[core, source],
                fwd_sem.at[0, k],
                fwd_sem.at[1, k],
                partner,
            )
        )

    for i in range(5, 7):
        loads[i].wait()
    for copy in hid_fwd:
        copy.wait()
    down = jnp.dot(hidden[0].reshape(128, HALF), down_w[0], preferred_element_type=F32)
    down = down + jnp.dot(hidden[1].reshape(128, HALF), down_w[1], preferred_element_type=F32)
    down = down.reshape(8, 16, 512)
    down_own[...] = down
    down_tx[...] = down.astype(BF16)
    gy_copies = [
        send(
            down_tx.at[(gy + k) % 8],
            down_rx.at[k - 1],
            gy_sem.at[0, k - 1],
            gy_sem.at[1, k - 1],
            columns[k - 1],
        )
        for k in range(1, 8)
    ]
    loads[7].wait()
    row = down_own[gy] + resid_ref[...].astype(F32)
    for k in range(7):
        gy_copies[k].wait()
        row = row + down_rx[k].astype(F32)

    for copies in w_sends:
        wait_all(copies)
    crossed = gy + 1 - 2 * x_hi
    from_down = (z + 3) % 4 * 2 + x_hi
    from_up = (z + 1) % 4 * 2 + x_hi
    w_sends = [
        spread(crossed, None, 3, z_up),
        spread(crossed, None, 4, z_down),
        spread(from_down, 0, 5, z_up),
        spread(from_up, 1, 6, z_down),
    ]
    for piece in (crossed, from_down, from_up):
        forward(piece)

    thinker_out = row.astype(BF16)
    for h in range(2):
        bridge_own[h] = jnp.dot(
            thinker_out, bridge_w[:, h * 1792 : (h + 1) * 1792], preferred_element_type=F32
        )
    pair = send(bridge_own.at[other], bridge_rx, bp_sem.at[0], bp_sem.at[1], partner)
    pair.wait()
    summed = bridge_own[core] + bridge_rx[...]
    bridge_tx[...] = summed.astype(BF16)
    b_copies = [
        send(bridge_tx, bridge_peers.at[k], bc_sem.at[0, k], bc_sem.at[1, k], chips[k])
        for k in range(7)
    ]
    for k in range(7):
        b_copies[k].wait()
        summed = summed + bridge_peers[k].astype(F32)
    bridge_half[core] = summed.astype(BF16)
    last = send(
        bridge_half.at[core], bridge_half.at[core], bf_sem.at[0], bf_sem.at[1], partner
    )
    last.wait()
    out_ref[:, :1792] = bridge_half[0]
    out_ref[:, 1792:] = bridge_half[1]

    wait_all(w_sends[0])
    wait_all(w_sends[1])
    across_down = (z + 3) % 4 * 2 + 1 - x_hi
    across_up = (z + 1) % 4 * 2 + 1 - x_hi
    w_sends.append(spread(across_down, 0, 7, z_up))
    w_sends.append(spread(across_up, 1, 8, z_down))
    forward(across_down)
    forward(across_up)
    wait_all(w_sends[2])
    wait_all(w_sends[3])
    forward((z + 2) % 4 * 2 + x_hi)
    wait_all(w_sends[4])
    wait_all(w_sends[5])
    forward((z + 2) % 4 * 2 + 1 - x_hi)
    for copies in forwards:
        wait_all(copies)
    wait_all(own_outs)


def thinker(x, resid, gate_t, up_t, down, bridge_weight, wq_t, wk_t, wv_t):
    vmem = pl.BlockSpec(memory_space=pltpu.VMEM)
    hbm = pl.BlockSpec(memory_space=pl.ANY)
    dma = pltpu.SemaphoreType.DMA
    return pl.pallas_call(
        thinker_kernel,
        out_shape=(
            jax.ShapeDtypeStruct((16, 3584), BF16),
            jax.ShapeDtypeStruct((8, 224, 3584), BF16),
            jax.ShapeDtypeStruct((2, 8, 32, 3584), BF16),
        ),
        in_specs=[vmem, vmem] + [hbm] * 7,
        out_specs=(vmem, hbm, hbm),
        scratch_shapes=[
            pltpu.VMEM((2, HALF, 512), BF16),
            pltpu.VMEM((2, HALF, 512), BF16),
            pltpu.VMEM((2, HALF, 512), BF16),
            pltpu.VMEM((512, 3584), BF16),
            pltpu.VMEM((224, 3584), BF16),
            pltpu.VMEM((2, 32, 3584), BF16),
            pltpu.VMEM((8, 16, 2 * HALF), BF16),
            pltpu.VMEM((8, 16, 2 * HALF), F32),
            pltpu.VMEM((8, 16, 2 * HALF), BF16),
            pltpu.VMEM((7, 16, 2 * HALF), BF16),
            pltpu.VMEM((7, 16, 2 * HALF), BF16),
            pltpu.VMEM((2, 8, 16, HALF), BF16),
            pltpu.VMEM((8, 16, 512), F32),
            pltpu.VMEM((8, 16, 512), BF16),
            pltpu.VMEM((7, 16, 512), BF16),
            pltpu.VMEM((2, 16, 1792), F32),
            pltpu.VMEM((16, 1792), F32),
            pltpu.VMEM((16, 1792), BF16),
            pltpu.VMEM((7, 16, 1792), BF16),
            pltpu.VMEM((2, 16, 1792), BF16),
            dma((12,)),
            dma((2,)),
            dma((2, 7)),
            dma((2, 7)),
            dma((2, 8)),
            dma((2, 7)),
            dma((2,)),
            dma((2, 7)),
            dma((2,)),
            dma((4, 16)),
        ],
        compiler_params=pltpu.CompilerParams(
            collective_id=0, has_side_effects=True, vmem_limit_bytes=48 << 20
        ),
        cost_estimate=pl.CostEstimate(
            flops=10**9, bytes_accessed=20 << 20, transcendentals=0
        ),
        name="thinker",
    )(x, resid, gate_t, up_t, down, bridge_weight, wq_t, wk_t, wv_t)


WIDTHS = (3584, 3584, 1792, 256)
PIECE = 1152


def segments():
    start = 0
    for which, width in enumerate(WIDTHS):
        done = 0
        while done < width:
            at = start + done
            chunk, offset = divmod(at, PIECE)
            size = min(width - done, PIECE - offset)
            yield which, done, chunk, offset, size
            done += size
        start += width


def talker_kernel(
    normal_ref,
    aq_ref,
    av_ref,
    wq_ref,
    wkv_ref,
    bq_ref,
    bv_ref,
    cos_ref,
    sin_ref,
    lim_ref,
    og_ref,
    attn_ref,
    gaq_ref,
    gav_ref,
    gbq_ref,
    gbv_ref,
    wkv,
    wq,
    low_s,
    kv,
    query,
    score,
    expo,
    dvt,
    qgrad,
    dl_tx,
    dl_rx,
    p_aq,
    p_av,
    p_bq,
    p_bv,
    packed,
    pair_rx,
    chip_tx,
    chip_rx,
    column,
    gathered,
    load_sem,
    kv_sem,
    kvf_sem,
    dl_sem,
    pair_sem,
    chip_sem,
    gy_sem,
    ag_sem,
    fwd_sem,
):
    gx, gy, chip, core = place()
    other = 1 - core
    partner = (chip * 2 + other, gy)
    chips = [((chip + k) % 8 * 2 + core, gy) for k in range(1, 8)]
    columns = [(gx, (gy + k) % 8) for k in range(1, 8)]
    row = [((gx + k) % 16, gy) for k in range(1, 16)]

    kv_load = pltpu.make_async_copy(wkv_ref, wkv, load_sem.at[0])
    kv_load.start()
    for i in range(7):
        pltpu.make_async_copy(wq_ref.at[i], wq.at[i], load_sem.at[1 + i]).start()
    greet(row + columns)

    normal = normal_ref[...]
    low_q = dot_nt(normal, aq_ref[...]).astype(BF16)
    low_v = dot_nt(normal, av_ref[...]).astype(BF16)
    low_s[:, :64] = low_q
    low_s[:, 64:] = low_v
    cosine = cos_ref[...]
    sine = sin_ref[...]
    kv_load.wait()
    keys = dot_nt(normal, wkv[:256])
    values = dot_nt(normal, wkv[256:]) + jnp.dot(
        low_v, bv_ref[...], preferred_element_type=F32
    )
    for g in range(KVH):
        head = keys[:, g * HD : (g + 1) * HD]
        kv[chip, core, :, g * HD : (g + 1) * HD] = (
            head * cosine + pltpu.roll(head, 64, 1) * sine
        ).astype(BF16)
    kv[chip, core, :, 256:512] = values.astype(BF16)
    kv[chip, core, :, 512:] = low_s[...]
    kv_copies = [
        send(kv.at[chip, core], kv.at[chip, core], kv_sem.at[0, k], kv_sem.at[1, k], chips[k])
        for k in range(7)
    ]
    kv_fwd = [
        send(kv.at[chip, core], kv.at[chip, core], kvf_sem.at[0, 7], kvf_sem.at[1, 7], partner)
    ]

    def project(i, carry):
        pltpu.make_async_copy(wq_ref.at[i], wq.at[i], load_sem.at[1 + i]).wait()
        at = pl.ds(pl.multiple_of(i * 256, 128), 256)
        pre = dot_nt(normal_ref[...], wq[i]) + jnp.dot(
            low_s[:, :64], bq_ref[:, at], preferred_element_type=F32
        )
        for t in range(2):
            head = pre[:, t * HD : (t + 1) * HD]
            query[2 * i + t] = (
                head * cos_ref[...] + pltpu.roll(head, 64, 1) * sin_ref[...]
            ).astype(BF16)
        return carry

    lax.fori_loop(0, 7, project, 0)
    dvt[...] = jnp.zeros_like(dvt)
    for k in range(7):
        kv_copies[k].wait()
        source = (chip + 7 - k) % 8
        kv_fwd.append(
            send(
                kv.at[source, core],
                kv.at[source, core],
                kvf_sem.at[0, k],
                kvf_sem.at[1, k],
                partner,
            )
        )
    for copy in kv_fwd:
        copy.wait()

    scale = 1.0 / math.sqrt(HD)
    fold = scale * math.log2(math.e)
    span = 768

    def keys_at(group, j):
        at = pl.ds(pl.multiple_of(group * HD, 128), HD)
        return kv[2 * j : 2 * j + 2, :, :, at].reshape(span, HD)

    def values_at(group, j):
        at = pl.ds(pl.multiple_of(256 + group * HD, 128), HD)
        return kv[2 * j : 2 * j + 2, :, :, at].reshape(span, HD)

    def attend(h, carry):
        group = h // 7
        at = pl.ds(pl.multiple_of(h * HD, 128), HD)
        q = query[h]
        lim = lim_ref[...]
        top = jnp.full((192, HD), -jnp.inf, F32)
        for j in range(4):
            s = dot_nt(q, keys_at(group, j))
            spot = lax.broadcasted_iota(jnp.int32, (192, span), 1) + j * span
            s = jnp.where(spot <= lim, s, -1e30)
            score[:, j * span : (j + 1) * span] = s
            for t in range(span // HD):
                top = jnp.maximum(top, s[:, t * HD : (t + 1) * HD])
        peak = jnp.max(top, axis=1, keepdims=True) * fold
        mass = jnp.zeros((192, HD), F32)
        out = jnp.zeros((192, HD), F32)
        for j in range(4):
            e = jnp.exp2(score[:, j * span : (j + 1) * span] * fold - peak)
            for t in range(span // HD):
                mass = mass + e[:, t * HD : (t + 1) * HD]
            e = e.astype(BF16)
            expo[:, j * span : (j + 1) * span] = e
            out = out + jnp.dot(e, values_at(group, j), preferred_element_type=F32)
        inverse = 1.0 / jnp.sum(mass, axis=1, keepdims=True)
        out = (out * inverse).astype(BF16)
        attn_ref[:, at] = out
        cot = og_ref[:, at]
        wide = cot.astype(F32)
        inner = jnp.sum(wide * out.astype(F32), axis=1, keepdims=True)
        turned = jnp.transpose(wide * inverse).astype(BF16)
        dq = jnp.zeros((192, HD), F32)
        for j in range(4):
            e = expo[:, j * span : (j + 1) * span]
            dp = dot_nt(cot, values_at(group, j))
            ds = (e.astype(F32) * (dp - inner)).astype(BF16)
            dq = dq + jnp.dot(ds, keys_at(group, j), preferred_element_type=F32)
            dvt[group, :, j * span : (j + 1) * span] += jnp.dot(
                turned, e, preferred_element_type=F32
            )
        dq = dq * (inverse * scale)
        qgrad[:, at] = (dq * cos_ref[...] - pltpu.roll(dq, 64, 1) * sin_ref[...]).astype(BF16)
        return carry

    lax.fori_loop(0, HEADS, attend, 0)

    for j in range(8):
        at = slice(384 * j, 384 * j + 384)
        part = jnp.dot(
            bv_ref[:, :HD], dvt[0, :, at].astype(BF16), preferred_element_type=F32
        ) + jnp.dot(bv_ref[:, HD:], dvt[1, :, at].astype(BF16), preferred_element_type=F32)
        dl_tx[2 * j] = part[:, :192].astype(BF16)
        dl_tx[2 * j + 1] = pltpu.roll(part, 192, 1)[:, :192].astype(BF16)
    dl_copies = [
        send(
            dl_tx.at[(gx + k) % 16],
            dl_rx.at[k - 1],
            dl_sem.at[0, k - 1],
            dl_sem.at[1, k - 1],
            row[k - 1],
        )
        for k in range(1, 16)
    ]
    for g in range(KVH):
        part = jnp.zeros((HD, HD), F32)
        for j in range(4):
            low = kv[2 * j : 2 * j + 2, :, :, 512:].reshape(span, HD)
            part = part + jnp.dot(
                dvt[g, :, j * span : (j + 1) * span].astype(BF16),
                low,
                preferred_element_type=F32,
            )
        p_bv[:, g * HD : (g + 1) * HD] = jnp.transpose(part)[64:]
    low_t = jnp.transpose(low_s[...].astype(F32)).astype(BF16)
    p_bq[...] = jnp.dot(low_t[:64], qgrad[...], preferred_element_type=F32)
    dlow_q = dot_nt(bq_ref[...], qgrad[...]).astype(BF16)
    p_aq[...] = jnp.dot(dlow_q, normal_ref[...], preferred_element_type=F32)
    dlow = dl_tx[gx].astype(F32)
    for k in range(15):
        dl_copies[k].wait()
        dlow = dlow + dl_rx[k].astype(F32)
    p_av[...] = jnp.dot(dlow.astype(BF16), normal_ref[...], preferred_element_type=F32)

    ins = (p_aq, p_av, p_bq, p_bv)
    outs = (gaq_ref, gav_ref, gbq_ref, gbv_ref)
    for which, done, chunk, offset, size in segments():
        for h in range(2):
            packed[h, chunk, :, offset : offset + size] = ins[which][
                32 * h : 32 * h + 32, done : done + size
            ].astype(BF16)
    pair = send(packed.at[other], pair_rx, pair_sem.at[0], pair_sem.at[1], partner)
    pair.wait()
    copies = []
    for k in range(1, 8):
        peer = (chip + k) % 8
        chip_tx[k - 1] = (packed[core, peer].astype(F32) + pair_rx[peer].astype(F32)).astype(BF16)
        copies.append(
            send(
                chip_tx.at[k - 1],
                chip_rx.at[k - 1],
                chip_sem.at[0, k - 1],
                chip_sem.at[1, k - 1],
                chips[k - 1],
            )
        )
    total = packed[core, chip].astype(F32) + pair_rx[chip].astype(F32)
    for k in range(7):
        copies[k].wait()
        total = total + chip_rx[k].astype(F32)
    column[gy] = total.astype(BF16)
    copies = [
        send(column.at[gy], column.at[gy], gy_sem.at[0, k], gy_sem.at[1, k], columns[k])
        for k in range(7)
    ]
    for copy in copies:
        copy.wait()
    total = column[0].astype(F32)
    for k in range(1, 8):
        total = total + column[k].astype(F32)
    gathered[core, chip] = total.astype(BF16)
    copies = [
        send(
            gathered.at[core, chip],
            gathered.at[core, chip],
            ag_sem.at[0, k],
            ag_sem.at[1, k],
            chips[k],
        )
        for k in range(7)
    ]
    fwd = [
        send(
            gathered.at[core, chip],
            gathered.at[core, chip],
            fwd_sem.at[0, 7],
            fwd_sem.at[1, 7],
            partner,
        )
    ]
    for k in range(7):
        copies[k].wait()
        source = (chip + 7 - k) % 8
        fwd.append(
            send(
                gathered.at[core, source],
                gathered.at[core, source],
                fwd_sem.at[0, k],
                fwd_sem.at[1, k],
                partner,
            )
        )
    for copy in fwd:
        copy.wait()
    for which, done, chunk, offset, size in segments():
        for h in range(2):
            outs[which][32 * h : 32 * h + 32, done : done + size] = gathered[
                h, chunk, :, offset : offset + size
            ].astype(F32)


def talker(*args):
    vmem = pl.BlockSpec(memory_space=pltpu.VMEM)
    hbm = pl.BlockSpec(memory_space=pl.ANY)
    dma = pltpu.SemaphoreType.DMA
    return pl.pallas_call(
        talker_kernel,
        out_shape=(jax.ShapeDtypeStruct((192, 1792), BF16),)
        + tuple(jax.ShapeDtypeStruct((64, w), F32) for w in WIDTHS),
        in_specs=[vmem] * 3 + [hbm] * 2 + [vmem] * 6,
        out_specs=(vmem,) * 5,
        scratch_shapes=[
            pltpu.VMEM((512, 3584), BF16),
            pltpu.VMEM((7, 256, 3584), BF16),
            pltpu.VMEM((192, 128), BF16),
            pltpu.VMEM((8, 2, 192, 640), BF16),
            pltpu.VMEM((HEADS, 192, HD), BF16),
            pltpu.VMEM((192, 3072), F32),
            pltpu.VMEM((192, 3072), BF16),
            pltpu.VMEM((KVH, HD, 3072), F32),
            pltpu.VMEM((192, 1792), BF16),
            pltpu.VMEM((16, 64, 192), BF16),
            pltpu.VMEM((15, 64, 192), BF16),
            pltpu.VMEM((64, 3584), F32),
            pltpu.VMEM((64, 3584), F32),
            pltpu.VMEM((64, 1792), F32),
            pltpu.VMEM((64, 256), F32),
            pltpu.VMEM((2, 8, 32, PIECE), BF16),
            pltpu.VMEM((8, 32, PIECE), BF16),
            pltpu.VMEM((7, 32, PIECE), BF16),
            pltpu.VMEM((7, 32, PIECE), BF16),
            pltpu.VMEM((8, 32, PIECE), BF16),
            pltpu.VMEM((2, 8, 32, PIECE), BF16),
            dma((8,)),
            dma((2, 7)),
            dma((2, 8)),
            dma((2, 15)),
            dma((2,)),
            dma((2, 7)),
            dma((2, 7)),
            dma((2, 7)),
            dma((2, 8)),
        ],
        compiler_params=pltpu.CompilerParams(
            collective_id=1, has_side_effects=True, vmem_limit_bytes=60 << 20
        ),
        cost_estimate=pl.CostEstimate(
            flops=3 * 10**10, bytes_accessed=20 << 20, transcendentals=10**7
        ),
        name="talker",
    )(*args)


def on_device(
    thinker_normed,
    thinker_resid,
    gate_weight,
    up_weight,
    down_weight,
    bridge_weight,
    talker_stream,
    norm_gain,
    w_query,
    w_key,
    w_value,
    a_query,
    b_query,
    a_value,
    b_value,
    text_index,
    span_offset,
    out_grad,
):
    seq_count, rows_seq, columns = thinker_normed.shape
    bridge, all_q, all_kv = thinker(
        thinker_normed.reshape(seq_count * rows_seq, columns),
        thinker_resid[0],
        gate_weight.T,
        up_weight.T,
        down_weight,
        bridge_weight,
        w_query.T,
        w_key.T,
        w_value.T,
    )
    tokens = talker_stream.shape[1]
    picks = (text_index[0][:, None] == jnp.arange(rows_seq, dtype=jnp.int32)[None, :]).astype(
        jnp.bfloat16
    )
    mixed = talker_stream[0].astype(jnp.float32) + jnp.dot(
        picks, bridge, preferred_element_type=jnp.float32
    )
    normal = (
        mixed * lax.rsqrt(jnp.mean(mixed * mixed, axis=1, keepdims=True) + norm_eps) * norm_gain
    ).astype(jnp.bfloat16)
    first_pos = lax.axis_index("gx") * tokens
    cosine, sine = angle_tables(first_pos, tokens)
    places = first_pos + jnp.arange(tokens, dtype=jnp.int32)
    limit = jnp.maximum(places, span_offset[0] - 1)[:, None]
    attn_out, grad_aq, grad_av, grad_bq, grad_bv = talker(
        normal,
        a_query.T,
        a_value.T,
        all_q.reshape(7, 256, 3584),
        all_kv.reshape(KVH * HD * 2, 3584),
        b_query,
        b_value,
        jnp.concatenate([cosine, cosine], axis=1),
        jnp.concatenate([-sine, sine], axis=1),
        limit,
        out_grad[0],
    )
    return (attn_out[None], grad_aq.T, grad_bq, grad_av.T, grad_bv)


def solution(mesh):
    return jax.shard_map(
        on_device,
        mesh=mesh,
        in_specs=(
            P(None, None, "gx"),
            P("gy", None, "gx"),
            P("gx", "gy"),
            P("gx", "gy"),
            P("gy", "gx"),
            P("gx", None),
            P("gy", "gx", None),
            P(),
            P(None, "gy"),
            P(None, "gy"),
            P(None, "gy"),
            P(),
            P(),
            P(),
            P(),
            P("gy", "gx"),
            P("gy"),
            P("gy", "gx", None),
        ),
        out_specs=(P("gy", "gx", None), P(), P(), P(), P()),
        check_vma=False,
    )
```

```python
import functools
import math

import jax
import jax.numpy as jnp
from jax import lax
from jax.experimental import pallas as pl
from jax.experimental.pallas import tpu as pltpu
from jax.sharding import PartitionSpec as P

HEADS = 14
KVH = 2
HD = 128
MESH = pl.DeviceIdType.MESH
F32 = jnp.float32
BF16 = jnp.bfloat16

rope_base = 1000000.0
norm_eps = 1e-06


def angle_tables(first_pos, length):
    position = (first_pos + jnp.arange(length, dtype=jnp.int32)).astype(jnp.float32)
    frequency = rope_base ** (-(2.0 * jnp.arange(HD // 2, dtype=jnp.float32)) / HD)
    angles = position[:, None] * frequency[None, :]
    return (jnp.cos(angles), jnp.sin(angles))


def place():
    gx = lax.axis_index("gx")
    gy = lax.axis_index("gy")
    return gx, gy, gx // 2, gx % 2


def greet(peers):
    barrier = pltpu.get_barrier_semaphore()
    for peer in peers:
        pl.semaphore_signal(barrier, inc=1, device_id=peer, device_id_type=MESH)
    pl.semaphore_wait(barrier, len(peers))


def remote(src, dst, send_sem, recv_sem, peer):
    return pltpu.make_async_remote_copy(
        src_ref=src,
        dst_ref=dst,
        send_sem=send_sem,
        recv_sem=recv_sem,
        device_id=peer,
        device_id_type=MESH,
    )


def send(*args):
    copy = remote(*args)
    copy.start()
    return copy


def dot_nt(a, b):
    return lax.dot_general(a, b, (((1,), (1,)), ((), ())), preferred_element_type=F32)


HALF = 1920
REST = 1776
CHUNK = 640
GROUPS = (
    (768, (("aq", 3584), ("bq", 1792), ("bv", 256))),
    (512, (("av", 3584),)),
)


def segments(group):
    piece, parts = GROUPS[group]
    start = 0
    for name, width in parts:
        done = 0
        while done < width:
            chunk, offset = divmod(start + done, piece)
            size = min(width - done, piece - offset)
            yield name, done, chunk, offset, size
            done += size
        start += width
    if start < 8 * piece:
        chunk, offset = divmod(start, piece)
        while chunk < 8:
            yield None, 0, chunk, offset, piece - offset
            chunk, offset = chunk + 1, 0


class Box:
    pass


INPUTS = [
    "x", "resid", "gate", "up", "down", "bridge", "wq", "wk", "wv", "stream", "og", "a_q",
    "a_v", "b_q", "b_v", "gain", "index", "cos", "sin", "lim",
]
OUTPUTS = ["attn", "aq", "av", "bq", "bv"]


def dma(*shape):
    return pltpu.SemaphoreType.DMA(shape)


def shared_scratch():
    vmem = pltpu.VMEM
    table = dict(
        all_q=vmem((1792, 3584), BF16),
        all_kv=vmem((2, 256, 3584), BF16),
        x_v=vmem((128, 512), BF16),
        resid_v=vmem((16, 512), BF16),
        stream_v=vmem((192, 3584), BF16),
        og_v=vmem((192, 1792), BF16),
        a_v_q=vmem((64, 3584), BF16),
        a_v_v=vmem((64, 3584), BF16),
        b_v_q=vmem((64, 1792), BF16),
        b_v_v=vmem((64, 256), BF16),
        pair_tx=vmem((8, 16, 2 * HALF), BF16),
        pair_rx=vmem((8, 16, 2 * HALF), BF16),
        chip_tx=vmem((7, 16, 2 * HALF), BF16),
        chip_rx=vmem((7, 16, 2 * HALF), BF16),
        hidden=vmem((2, 8, 16, HALF), BF16),
        down_tx=vmem((8, 16, 512), BF16),
        down_rx=vmem((7, 16, 512), BF16),
        bridge_own=vmem((2, 16, 1792), F32),
        bridge_rx=vmem((16, 1792), F32),
        bridge_tx=vmem((16, 1792), BF16),
        bridge_peers=vmem((7, 16, 1792), BF16),
        bridge_half=vmem((2, 16, 1792), BF16),
        kv=vmem((8, 2, 192, 512), BF16),
        low=vmem((8, 2, 192, 128), BF16),
        dl_tx=vmem((16, 64, 192), BF16),
        dl_rx=vmem((15, 64, 192), BF16),
        load_sem=dma(18),
        pair_sem=dma(2),
        chip_sem=dma(2, 7),
        hid_sem=dma(2, 7),
        hidf_sem=dma(2, 8),
        gy_sem=dma(2, 7),
        bp_sem=dma(2),
        bc_sem=dma(2, 7),
        bf_sem=dma(2),
        wq_sem=dma(2, 16),
        wkv_sem=dma(2, 16),
        kv_sem=dma(2, 7),
        kvf_sem=dma(2, 8),
        low_sem=dma(2, 7),
        lowf_sem=dma(2, 8),
        dl_sem=dma(2, 15),
    )
    for n, (piece, _) in enumerate(GROUPS):
        table.update(
            {
                f"packed{n}": vmem((2, 8, 32, piece), BF16),
                f"g_pair{n}": vmem((8, 32, piece), BF16),
                f"g_tx{n}": vmem((7, 32, piece), BF16),
                f"g_rx{n}": vmem((7, 32, piece), BF16),
                f"y_tx{n}": vmem((8, 4, piece), F32),
                f"y_rx{n}": vmem((7, 4, piece), F32),
                f"y_all{n}": vmem((8, 4, piece), F32),
                f"g_all{n}": vmem((2, 8, 32, piece), BF16),
                f"gp_sem{n}": dma(2),
                f"gc_sem{n}": dma(2, 7),
                f"gy1_sem{n}": dma(2, 7),
                f"gy2_sem{n}": dma(2, 7),
                f"ga_sem{n}": dma(2, 7),
                f"gf_sem{n}": dma(2, 8),
            }
        )
    return table


THINKER = dict(
    gate_w=pltpu.VMEM((2, HALF, 512), BF16),
    up_w=pltpu.VMEM((2, HALF, 512), BF16),
    down_w=pltpu.VMEM((2, HALF, 512), BF16),
    bridge_w=pltpu.VMEM((512, 3584), BF16),
    own_half=pltpu.VMEM((8, 16, 2 * HALF), F32),
    down_own=pltpu.VMEM((8, 16, 512), F32),
)
TALKER = dict(
    mixed=pltpu.VMEM((192, 3584), F32),
    normal=pltpu.VMEM((192, 3584), BF16),
    query=pltpu.VMEM((HEADS, 192, HD), BF16),
    score=pltpu.VMEM((192, 3072), F32),
    expo=pltpu.VMEM((192, 3072), BF16),
    dvt=pltpu.VMEM((KVH, HD, 3072), F32),
    qgrad=pltpu.VMEM((192, 1792), BF16),
    p_aq=pltpu.VMEM((64, 3584), F32),
    p_av=pltpu.VMEM((64, 3584), F32),
    p_bq=pltpu.VMEM((64, 1792), F32),
    p_bv=pltpu.VMEM((64, 256), F32),
)


def weight_copy(r, kind, n):
    gx, gy, chip, core = place()
    z = gy // 2
    x_hi = gy % 2
    flip = 1 - x_hi
    up, down, far = (z + 1) % 4 * 2, (z + 3) % 4 * 2, (z + 2) % 4 * 2
    cross = ((chip + 1 - 2 * (chip % 2)) * 2 + core, z * 2 + flip)
    z_up, z_down = (gx, up + x_hi), (gx, down + x_hi)
    partner = (chip * 2 + 1 - core, gy)
    piece, part, peer = (
        (gy, None, cross),
        (gy, None, z_up),
        (gy, None, z_down),
        (z * 2 + flip, None, z_up),
        (z * 2 + flip, None, z_down),
        (down + x_hi, 0, z_up),
        (up + x_hi, 1, z_down),
        (down + flip, 0, z_up),
        (up + flip, 1, z_down),
        (z * 2 + flip, None, partner),
        (down + x_hi, None, partner),
        (up + x_hi, None, partner),
        (down + flip, None, partner),
        (up + flip, None, partner),
        (far + x_hi, None, partner),
        (far + flip, None, partner),
    )[n]
    cols = pl.ds(pl.multiple_of(core * 1792, 128), 1792)
    if kind == "q":
        rows = 224 if part is None else 112
        first = pl.multiple_of(piece * 224 + (0 if part is None else 112 * part), 16)
        ref, sem = r.all_q.at[pl.ds(first, rows), cols], r.wq_sem
    else:
        kinds = pl.ds(0, 2) if part is None else pl.ds(part, 1)
        rows = pl.ds(pl.multiple_of(piece * 32, 32), 32)
        ref, sem = r.all_kv.at[kinds, rows, cols], r.wkv_sem
    return remote(ref, ref, sem.at[0, n], sem.at[1, n], peer)


def weights_go(r, kind, *numbers):
    for n in numbers:
        weight_copy(r, kind, n).start()


def weights_wait(r, kind, *numbers):
    for n in numbers:
        weight_copy(r, kind, n).wait()


def early_loads(r):
    gy = lax.axis_index("gy")
    rows = pl.ds(pl.multiple_of(gy * 32, 32), 32)
    plan = [
        (r.wk, r.all_kv.at[0, rows]),
        (r.wv, r.all_kv.at[1, rows]),
        (r.wq, r.all_q.at[pl.ds(pl.multiple_of(gy * 224, 32), 224)]),
        (r.x, r.x_v),
        (r.resid, r.resid_v),
    ]
    return [pltpu.make_async_copy(a, b, r.load_sem.at[i]) for i, (a, b) in enumerate(plan)]


def late_loads(r):
    plan = [
        (r.stream, r.stream_v),
        (r.a_q, r.a_v_q),
        (r.a_v, r.a_v_v),
        (r.b_q, r.b_v_q),
        (r.b_v, r.b_v_v),
        (r.og, r.og_v),
    ]
    return [pltpu.make_async_copy(a, b, r.load_sem.at[5 + i]) for i, (a, b) in enumerate(plan)]


def think(r):
    gx, gy, chip, core = place()
    other = 1 - core
    partner = (chip * 2 + other, gy)
    chips = [((chip + k) % 8 * 2 + core, gy) for k in range(1, 8)]
    columns = [(gx, (gy + k) % 8) for k in range(1, 8)]
    row = [((gx + k) % 16, gy) for k in range(1, 16)]
    cross = ((chip + 1 - 2 * (chip % 2)) * 2 + core, gy + 1 - 2 * (gy % 2))

    first = early_loads(r)
    for copy in first:
        copy.start()
    plan = [
        (r.gate.at[pl.ds(0, HALF)], r.gate_w.at[0]),
        (r.gate.at[pl.ds(HALF, REST)], r.gate_w.at[1, pl.ds(0, REST)]),
        (r.up.at[pl.ds(0, HALF)], r.up_w.at[0]),
        (r.up.at[pl.ds(HALF, REST)], r.up_w.at[1, pl.ds(0, REST)]),
        (r.down.at[pl.ds(0, HALF)], r.down_w.at[0]),
        (r.down.at[pl.ds(HALF, REST)], r.down_w.at[1, pl.ds(0, REST)]),
        (r.bridge, r.bridge_w),
    ]
    loads = [pltpu.make_async_copy(a, b, r.load_sem.at[11 + i]) for i, (a, b) in enumerate(plan)]
    for copy in loads:
        copy.start()
    for copy in late_loads(r):
        copy.start()
    pad = jnp.zeros((HALF - REST, 512), BF16)
    r.gate_w[1, REST:] = pad
    r.up_w[1, REST:] = pad
    r.down_w[1, REST:] = pad

    greet(row + columns + [cross])

    first[0].wait()
    first[1].wait()
    weights_go(r, "kv", 0, 1, 2)
    first[2].wait()
    weights_go(r, "q", 0, 1, 2)

    first[3].wait()
    first[4].wait()
    for copy in loads[:4]:
        copy.wait()
    x = r.x_v[...]
    for half, is_own in ((other, False), (core, True)):
        for side, weight in ((0, r.gate_w), (1, r.up_w)):
            for c in range(HALF // CHUNK):
                part = dot_nt(x, weight[half, c * CHUNK : (c + 1) * CHUNK])
                part = part.reshape(8, 16, CHUNK)
                lo = side * HALF + c * CHUNK
                if is_own:
                    r.own_half[:, :, lo : lo + CHUNK] = part
                else:
                    r.pair_tx[:, :, lo : lo + CHUNK] = part.astype(BF16)
        if not is_own:
            pair_copy = send(r.pair_tx, r.pair_rx, r.pair_sem.at[0], r.pair_sem.at[1], partner)
    pair_copy.wait()

    chip_copies = []
    for k in range(1, 8):
        peer = (chip + k) % 8
        r.chip_tx[k - 1] = (r.own_half[peer] + r.pair_rx[peer].astype(F32)).astype(BF16)
        chip_copies.append(
            send(
                r.chip_tx.at[k - 1],
                r.chip_rx.at[k - 1],
                r.chip_sem.at[0, k - 1],
                r.chip_sem.at[1, k - 1],
                chips[k - 1],
            )
        )
    total = r.own_half[chip] + r.pair_rx[chip].astype(F32)
    for k in range(7):
        chip_copies[k].wait()
        total = total + r.chip_rx[k].astype(F32)
    gate = total[:, :HALF]
    r.hidden[core, chip] = (gate / (1.0 + jnp.exp(-gate)) * total[:, HALF:]).astype(BF16)

    fan_out(r.hidden, r.hid_sem, chip, core, chips)
    finish = relay_to_partner(r.hidden, r.hid_sem, r.hidf_sem, chip, core, chips, partner)
    loads[4].wait()
    loads[5].wait()
    finish()
    down = jnp.dot(r.hidden[0].reshape(128, HALF), r.down_w[0], preferred_element_type=F32)
    down = down + jnp.dot(
        r.hidden[1].reshape(128, HALF), r.down_w[1], preferred_element_type=F32
    )
    down = down.reshape(8, 16, 512)
    r.down_own[...] = down
    r.down_tx[...] = down.astype(BF16)
    gy_copies = [
        send(
            r.down_tx.at[(gy + k) % 8],
            r.down_rx.at[k - 1],
            r.gy_sem.at[0, k - 1],
            r.gy_sem.at[1, k - 1],
            columns[k - 1],
        )
        for k in range(1, 8)
    ]
    weights_wait(r, "kv", 0, 1, 2)
    weights_go(r, "kv", 3, 4, 5, 6, 9, 10, 11)
    loads[6].wait()
    tokens = r.down_own[gy] + r.resid_v[...].astype(F32)
    for k in range(7):
        gy_copies[k].wait()
        tokens = tokens + r.down_rx[k].astype(F32)
    weights_wait(r, "q", 0, 1, 2)
    weights_go(r, "q", 5, 6, 9, 10, 11)

    thinker_out = tokens.astype(BF16)
    for h in range(2):
        r.bridge_own[h] = jnp.dot(
            thinker_out, r.bridge_w[:, h * 1792 : (h + 1) * 1792], preferred_element_type=F32
        )
    send(r.bridge_own.at[other], r.bridge_rx, r.bp_sem.at[0], r.bp_sem.at[1], partner).wait()
    summed = r.bridge_own[core] + r.bridge_rx[...]
    r.bridge_tx[...] = summed.astype(BF16)
    b_copies = [
        send(r.bridge_tx, r.bridge_peers.at[k], r.bc_sem.at[0, k], r.bc_sem.at[1, k], chips[k])
        for k in range(7)
    ]
    weights_wait(r, "kv", 3, 4)
    weights_go(r, "kv", 7, 8, 12, 13)
    weights_go(r, "q", 3, 4)
    for k in range(7):
        b_copies[k].wait()
        summed = summed + r.bridge_peers[k].astype(F32)
    r.bridge_half[core] = summed.astype(BF16)
    send(
        r.bridge_half.at[core], r.bridge_half.at[core], r.bf_sem.at[0], r.bf_sem.at[1], partner
    ).wait()


def fan_out(ref, sem, chip, core, chips):
    here = ref.at[chip, core] if ref.shape[0] == 8 else ref.at[core, chip]
    for k in range(7):
        send(here, here, sem.at[0, k], sem.at[1, k], chips[k])


def relay_to_partner(ref, sem, fwd_sem, chip, core, chips, partner):
    def at(which):
        return ref.at[which, core] if ref.shape[0] == 8 else ref.at[core, which]

    here = at(chip)
    passed = [send(here, here, fwd_sem.at[0, 7], fwd_sem.at[1, 7], partner)]
    for k in range(7):
        remote(here, here, sem.at[0, k], sem.at[1, k], chips[k]).wait()
        block = at((chip + 7 - k) % 8)
        passed.append(send(block, block, fwd_sem.at[0, k], fwd_sem.at[1, k], partner))

    def finish():
        for copy in passed:
            copy.wait()

    return finish


def reduce_group(r, n, parts, outs):
    gx, gy, chip, core = place()
    other = 1 - core
    partner = (chip * 2 + other, gy)
    chips = [((chip + k) % 8 * 2 + core, gy) for k in range(1, 8)]
    columns = [(gx, (gy + k) % 8) for k in range(1, 8)]

    def own(name):
        return getattr(r, f"{name}{n}")

    packed, g_pair, g_tx, g_rx = own("packed"), own("g_pair"), own("g_tx"), own("g_rx")
    y_tx, y_rx, y_all, g_all = own("y_tx"), own("y_rx"), own("y_all"), own("g_all")
    for name, done, chunk, offset, size in segments(n):
        for h in range(2):
            if name is None:
                packed[h, chunk, :, offset : offset + size] = jnp.zeros((32, size), BF16)
            else:
                packed[h, chunk, :, offset : offset + size] = parts[name][
                    32 * h : 32 * h + 32, done : done + size
                ].astype(BF16)
    sem = own("gp_sem")
    pair = send(packed.at[other], g_pair, sem.at[0], sem.at[1], partner)
    yield
    pair.wait()
    sem = own("gc_sem")
    copies = []
    for k in range(1, 8):
        peer = (chip + k) % 8
        g_tx[k - 1] = (packed[core, peer].astype(F32) + g_pair[peer].astype(F32)).astype(BF16)
        copies.append(
            send(g_tx.at[k - 1], g_rx.at[k - 1], sem.at[0, k - 1], sem.at[1, k - 1], chips[k - 1])
        )
    total = packed[core, chip].astype(F32) + g_pair[chip].astype(F32)
    yield
    for k in range(7):
        copies[k].wait()
        total = total + g_rx[k].astype(F32)
    for i in range(8):
        y_tx[i] = total[4 * i : 4 * i + 4]
    sem = own("gy1_sem")
    copies = [
        send(
            y_tx.at[(gy + k) % 8], y_rx.at[k - 1], sem.at[0, k - 1], sem.at[1, k - 1], columns[k - 1]
        )
        for k in range(1, 8)
    ]
    total = y_tx[gy]
    yield
    for k in range(7):
        copies[k].wait()
        total = total + y_rx[k]
    y_all[gy] = total
    sem = own("gy2_sem")
    copies = [
        send(y_all.at[gy], y_all.at[gy], sem.at[0, k], sem.at[1, k], columns[k]) for k in range(7)
    ]
    yield
    for copy in copies:
        copy.wait()
    g_all[core, chip] = jnp.concatenate([y_all[i] for i in range(8)], axis=0).astype(BF16)
    fan_out(g_all, own("ga_sem"), chip, core, chips)
    yield
    finish = relay_to_partner(g_all, own("ga_sem"), own("gf_sem"), chip, core, chips, partner)
    yield
    finish()
    for name, done, chunk, offset, size in segments(n):
        if name is not None:
            for h in range(2):
                outs[name][32 * h : 32 * h + 32, done : done + size] = g_all[
                    h, chunk, :, offset : offset + size
                ].astype(F32)


def talk(r):
    gx, gy, chip, core = place()
    other = 1 - core
    partner = (chip * 2 + other, gy)
    chips = [((chip + k) % 8 * 2 + core, gy) for k in range(1, 8)]
    row = [((gx + k) % 16, gy) for k in range(1, 16)]
    kv = r.kv

    for copy in late_loads(r):
        copy.wait()
    picks = (r.index[...] == lax.broadcasted_iota(jnp.int32, (192, 16), 1)).astype(BF16)
    squares = jnp.zeros((192, HD), F32)
    for c in range(7):
        at = slice(512 * c, 512 * c + 512)
        pieces = []
        for lo, hi in ((512 * c, 512 * c + 256), (512 * c + 256, 512 * c + 512)):
            half, off = divmod(lo, 1792)
            pieces.append(r.bridge_half[half, :, off : off + 256])
        rows = jnp.concatenate(pieces, axis=1)
        mix = r.stream_v[:, at].astype(F32) + jnp.dot(picks, rows, preferred_element_type=F32)
        r.mixed[:, at] = mix
        for t in range(4):
            m = mix[:, t * HD : (t + 1) * HD]
            squares = squares + m * m
    rate = lax.rsqrt(jnp.sum(squares, axis=1, keepdims=True) / 3584.0 + norm_eps)
    for c in range(7):
        at = slice(512 * c, 512 * c + 512)
        r.normal[:, at] = (r.mixed[:, at] * rate * r.gain[:, at]).astype(BF16)

    normal = r.normal[...]
    low_q = dot_nt(normal, r.a_v_q[...]).astype(BF16)
    low_v = dot_nt(normal, r.a_v_v[...]).astype(BF16)
    r.low[chip, core, :, :64] = low_q
    r.low[chip, core, :, 64:] = low_v
    weights_wait(r, "kv", 5, 6)
    weights_go(r, "kv", 14)
    weights_wait(r, "kv", 7, 8)
    weights_go(r, "kv", 15)
    weights_wait(r, "kv", *range(9, 16))
    keys = dot_nt(normal, r.all_kv[0])
    values = dot_nt(normal, r.all_kv[1]) + jnp.dot(
        low_v, r.b_v_v[...], preferred_element_type=F32
    )
    for g in range(KVH):
        head = keys[:, g * HD : (g + 1) * HD]
        kv[chip, core, :, g * HD : (g + 1) * HD] = (
            head * r.cos[...] + pltpu.roll(head, 64, 1) * r.sin[...]
        ).astype(BF16)
    kv[chip, core, :, 256:] = values.astype(BF16)
    fan_out(kv, r.kv_sem, chip, core, chips)
    fan_out(r.low, r.low_sem, chip, core, chips)
    r.dvt[...] = jnp.zeros_like(r.dvt)

    weights_wait(r, "q", 5, 6)
    weights_go(r, "q", 14)
    weights_wait(r, "q", 3, 4)
    weights_go(r, "q", 7, 8, 12, 13)
    kv_finish = relay_to_partner(kv, r.kv_sem, r.kvf_sem, chip, core, chips, partner)
    weights_wait(r, "q", 7, 8)
    weights_go(r, "q", 15)
    low_finish = relay_to_partner(r.low, r.low_sem, r.lowf_sem, chip, core, chips, partner)
    weights_wait(r, "q", *range(9, 16))

    def project(i, carry):
        at = pl.ds(pl.multiple_of(i * 256, 128), 256)
        pre = dot_nt(r.normal[...], r.all_q[at]) + jnp.dot(
            r.low[chip, core, :, :64], r.b_v_q[:, at], preferred_element_type=F32
        )
        for t in range(2):
            head = pre[:, t * HD : (t + 1) * HD]
            r.query[2 * i + t] = (
                head * r.cos[...] + pltpu.roll(head, 64, 1) * r.sin[...]
            ).astype(BF16)
        return carry

    lax.fori_loop(0, 7, project, 0)
    kv_finish()

    scale = 1.0 / math.sqrt(HD)
    fold = scale * math.log2(math.e)
    span = 768

    def keys_at(group, j):
        at = pl.ds(pl.multiple_of(group * HD, 128), HD)
        return kv[2 * j : 2 * j + 2, :, :, at].reshape(span, HD)

    def values_at(group, j):
        at = pl.ds(pl.multiple_of(256 + group * HD, 128), HD)
        return kv[2 * j : 2 * j + 2, :, :, at].reshape(span, HD)

    def attend(h, carry):
        group = h // 7
        at = pl.ds(pl.multiple_of(h * HD, 128), HD)
        q = r.query[h]
        lim = r.lim[...]
        top = jnp.full((192, HD), -jnp.inf, F32)
        for j in range(4):
            s = dot_nt(q, keys_at(group, j))
            spot = lax.broadcasted_iota(jnp.int32, (192, span), 1) + j * span
            s = jnp.where(spot <= lim, s, -1e30)
            r.score[:, j * span : (j + 1) * span] = s
            for t in range(span // HD):
                top = jnp.maximum(top, s[:, t * HD : (t + 1) * HD])
        peak = jnp.max(top, axis=1, keepdims=True) * fold
        mass = jnp.zeros((192, HD), F32)
        out = jnp.zeros((192, HD), F32)
        for j in range(4):
            e = jnp.exp2(r.score[:, j * span : (j + 1) * span] * fold - peak)
            for t in range(span // HD):
                mass = mass + e[:, t * HD : (t + 1) * HD]
            e = e.astype(BF16)
            r.expo[:, j * span : (j + 1) * span] = e
            out = out + jnp.dot(e, values_at(group, j), preferred_element_type=F32)
        inverse = 1.0 / jnp.sum(mass, axis=1, keepdims=True)
        out = (out * inverse).astype(BF16)
        r.attn[:, at] = out
        cot = r.og_v[:, at]
        wide = cot.astype(F32)
        inner = jnp.sum(wide * out.astype(F32), axis=1, keepdims=True)
        turned = jnp.transpose(wide * inverse).astype(BF16)
        dq = jnp.zeros((192, HD), F32)
        for j in range(4):
            e = r.expo[:, j * span : (j + 1) * span]
            dp = dot_nt(cot, values_at(group, j))
            ds = (e.astype(F32) * (dp - inner)).astype(BF16)
            dq = dq + jnp.dot(ds, keys_at(group, j), preferred_element_type=F32)
            r.dvt[group, :, j * span : (j + 1) * span] += jnp.dot(
                turned, e, preferred_element_type=F32
            )
        dq = dq * (inverse * scale)
        r.qgrad[:, at] = (dq * r.cos[...] - pltpu.roll(dq, 64, 1) * r.sin[...]).astype(BF16)
        return carry

    lax.fori_loop(0, HEADS, attend, 0)

    for j in range(8):
        at = slice(384 * j, 384 * j + 384)
        part = jnp.dot(
            r.b_v_v[:, :HD], r.dvt[0, :, at].astype(BF16), preferred_element_type=F32
        ) + jnp.dot(r.b_v_v[:, HD:], r.dvt[1, :, at].astype(BF16), preferred_element_type=F32)
        r.dl_tx[2 * j] = part[:, :192].astype(BF16)
        r.dl_tx[2 * j + 1] = pltpu.roll(part, 192, 1)[:, :192].astype(BF16)
    dl_copies = [
        send(
            r.dl_tx.at[(gx + k) % 16],
            r.dl_rx.at[k - 1],
            r.dl_sem.at[0, k - 1],
            r.dl_sem.at[1, k - 1],
            row[k - 1],
        )
        for k in range(1, 16)
    ]
    low_finish()
    low_t = jnp.transpose(r.low[chip, core].astype(F32)).astype(BF16)
    r.p_bq[...] = jnp.dot(low_t[:64], r.qgrad[...], preferred_element_type=F32)
    dlow_q = dot_nt(r.b_v_q[...], r.qgrad[...]).astype(BF16)
    r.p_aq[...] = jnp.dot(dlow_q, r.normal[...], preferred_element_type=F32)
    for g in range(KVH):
        part = jnp.zeros((HD, HD), F32)
        for j in range(4):
            low = r.low[2 * j : 2 * j + 2].reshape(span, HD)
            part = part + jnp.dot(
                r.dvt[g, :, j * span : (j + 1) * span].astype(BF16),
                low,
                preferred_element_type=F32,
            )
        r.p_bv[:, g * HD : (g + 1) * HD] = jnp.transpose(part)[64:]
    parts = dict(aq=r.p_aq, av=r.p_av, bq=r.p_bq, bv=r.p_bv)
    outs = dict(aq=r.aq, av=r.av, bq=r.bq, bv=r.bv)
    early = reduce_group(r, 0, parts, outs)
    next(early)
    next(early)
    dlow = r.dl_tx[gx].astype(F32)
    for k in range(15):
        dl_copies[k].wait()
        dlow = dlow + r.dl_rx[k].astype(F32)
    r.p_av[...] = jnp.dot(dlow.astype(BF16), r.normal[...], preferred_element_type=F32)
    late = reduce_group(r, 1, parts, outs)
    running = [late, early]
    while running:
        for group in list(running):
            if next(group, "end") == "end":
                running.remove(group)


def kernel(names, *refs):
    r = Box()
    for name, ref in zip(names, refs, strict=True):
        setattr(r, name, ref)

    def scoped(run, table):
        def inner(*more):
            box = Box()
            box.__dict__.update(r.__dict__)
            for name, ref in zip(table, more, strict=True):
                setattr(box, name, ref)
            run(box)

        pl.run_scoped(inner, *table.values())

    scoped(think, THINKER)
    scoped(talk, TALKER)


def whole(*args):
    vmem = pl.BlockSpec(memory_space=pltpu.VMEM)
    hbm = pl.BlockSpec(memory_space=pltpu.HBM)
    scratch = shared_scratch()
    names = INPUTS + OUTPUTS + list(scratch)
    return pl.pallas_call(
        functools.partial(kernel, names),
        out_shape=(
            jax.ShapeDtypeStruct((192, 1792), BF16),
            jax.ShapeDtypeStruct((64, 3584), F32),
            jax.ShapeDtypeStruct((64, 3584), F32),
            jax.ShapeDtypeStruct((64, 1792), F32),
            jax.ShapeDtypeStruct((64, 256), F32),
        ),
        in_specs=[hbm] * 15 + [vmem] * 5,
        out_specs=(vmem,) * 5,
        scratch_shapes=list(scratch.values()),
        compiler_params=pltpu.CompilerParams(
            collective_id=0, has_side_effects=True, vmem_limit_bytes=63 << 20
        ),
        name="layer",
    )(*args)


def on_device(
    thinker_normed,
    thinker_resid,
    gate_weight,
    up_weight,
    down_weight,
    bridge_weight,
    talker_stream,
    norm_gain,
    w_query,
    w_key,
    w_value,
    a_query,
    b_query,
    a_value,
    b_value,
    text_index,
    span_offset,
    out_grad,
):
    seq_count, rows_seq, columns = thinker_normed.shape
    tokens = talker_stream.shape[1]
    first_pos = lax.axis_index("gx") * tokens
    cosine, sine = angle_tables(first_pos, tokens)
    places = first_pos + jnp.arange(tokens, dtype=jnp.int32)
    limit = jnp.maximum(places, span_offset[0] - 1)[:, None]
    attn_out, grad_aq, grad_av, grad_bq, grad_bv = whole(
        thinker_normed.reshape(seq_count * rows_seq, columns),
        thinker_resid[0],
        gate_weight.T,
        up_weight.T,
        down_weight,
        bridge_weight,
        w_query.T,
        w_key.T,
        w_value.T,
        talker_stream[0],
        out_grad[0],
        a_query.T,
        a_value.T,
        b_query,
        b_value,
        norm_gain[None],
        text_index[0][:, None],
        jnp.concatenate([cosine, cosine], axis=1),
        jnp.concatenate([-sine, sine], axis=1),
        limit,
    )
    return (attn_out[None], grad_aq.T, grad_bq, grad_av.T, grad_bv)


def solution(mesh):
    return jax.shard_map(
        on_device,
        mesh=mesh,
        in_specs=(
            P(None, None, "gx"),
            P("gy", None, "gx"),
            P("gx", "gy"),
            P("gx", "gy"),
            P("gy", "gx"),
            P("gx", None),
            P("gy", "gx", None),
            P(),
            P(None, "gy"),
            P(None, "gy"),
            P(None, "gy"),
            P(),
            P(),
            P(),
            P(),
            P("gy", "gx"),
            P("gy"),
            P("gy", "gx", None),
        ),
        out_specs=(P("gy", "gx", None), P(), P(), P(), P()),
        check_vma=False,
    )
```

```python
import functools
import math

import jax
import jax.numpy as jnp
import numpy as np
from jax import lax
from jax.experimental import pallas as pl
from jax.experimental.pallas import tpu as pltpu
from jax.sharding import PartitionSpec as P

HEADS = 14
KVH = 2
HD = 128
MESH = pl.DeviceIdType.MESH
F32 = jnp.float32
BF16 = jnp.bfloat16

rope_base = 1000000.0
norm_eps = 1e-06


def place():
    gx = lax.axis_index("gx")
    gy = lax.axis_index("gy")
    return gx, gy, gx // 2, gx % 2


def greet(peers):
    barrier = pltpu.get_barrier_semaphore()
    for peer in peers:
        pl.semaphore_signal(barrier, inc=1, device_id=peer, device_id_type=MESH)
    pl.semaphore_wait(barrier, len(peers))


def remote(src, dst, send_sem, recv_sem, peer):
    return pltpu.make_async_remote_copy(
        src_ref=src,
        dst_ref=dst,
        send_sem=send_sem,
        recv_sem=recv_sem,
        device_id=peer,
        device_id_type=MESH,
    )


def send(*args):
    copy = remote(*args)
    copy.start()
    return copy


def dot_nt(a, b):
    return lax.dot_general(a, b, (((1,), (1,)), ((), ())), preferred_element_type=F32)


HALF = 1920
REST = 1776
CHUNK = 640
GROUPS = (
    (768, (("aq", 3584), ("bq", 1792), ("bv", 256))),
    (512, (("av", 3584),)),
)


def segments(group):
    piece, parts = GROUPS[group]
    start = 0
    for name, width in parts:
        done = 0
        while done < width:
            chunk, offset = divmod(start + done, piece)
            size = min(width - done, piece - offset)
            yield name, done, chunk, offset, size
            done += size
        start += width
    if start < 8 * piece:
        chunk, offset = divmod(start, piece)
        while chunk < 8:
            yield None, 0, chunk, offset, piece - offset
            chunk, offset = chunk + 1, 0


class Box:
    pass


INPUTS = [
    "x", "resid", "gate", "up", "down", "bridge", "wq", "wk", "wv", "stream", "og", "a_q",
    "a_v", "b_q", "b_v", "gain", "index", "freq", "offset",
]
OUTPUTS = ["attn", "aq", "av", "bq", "bv"]


def dma(*shape):
    return pltpu.SemaphoreType.DMA(shape)


def shared_scratch():
    vmem = pltpu.VMEM
    table = dict(
        all_q=vmem((1792, 3584), BF16),
        all_kv=vmem((2, 256, 3584), BF16),
        cos=vmem((192, 128), F32),
        sin=vmem((192, 128), F32),
        x_v=vmem((128, 512), BF16),
        resid_v=vmem((16, 512), BF16),
        stream_v=vmem((192, 3584), BF16),
        og_v=vmem((192, 1792), BF16),
        a_v_q=vmem((64, 3584), BF16),
        a_v_v=vmem((64, 3584), BF16),
        b_v_q=vmem((64, 1792), BF16),
        b_v_v=vmem((64, 256), BF16),
        pair_tx=vmem((8, 16, 2 * HALF), BF16),
        pair_rx=vmem((8, 16, 2 * HALF), BF16),
        chip_tx=vmem((7, 16, 2 * HALF), BF16),
        chip_rx=vmem((7, 16, 2 * HALF), BF16),
        hidden=vmem((2, 8, 16, HALF), BF16),
        down_tx=vmem((8, 16, 512), BF16),
        down_rx=vmem((7, 16, 512), BF16),
        bridge_own=vmem((2, 16, 1792), F32),
        bridge_rx=vmem((16, 1792), F32),
        bridge_tx=vmem((16, 1792), BF16),
        bridge_peers=vmem((7, 16, 1792), BF16),
        bridge_half=vmem((2, 16, 1792), BF16),
        kv=vmem((8, 2, 192, 512), BF16),
        low=vmem((8, 2, 192, 128), BF16),
        dl_tx=vmem((16, 64, 192), BF16),
        dl_rx=vmem((15, 64, 192), BF16),
        load_sem=dma(18),
        pair_sem=dma(2),
        chip_sem=dma(2, 7),
        hid_sem=dma(2, 7),
        hidf_sem=dma(2, 8),
        gy_sem=dma(2, 7),
        bp_sem=dma(2),
        bc_sem=dma(2, 7),
        bf_sem=dma(2),
        wq_sem=dma(2, 18),
        wkv_sem=dma(2, 16),
        kv_sem=dma(2, 7),
        kvf_sem=dma(2, 8),
        low_sem=dma(2, 7),
        lowf_sem=dma(2, 8),
        dl_sem=dma(2, 15),
        out_sem=dma(5),
    )
    for n, (piece, _) in enumerate(GROUPS):
        table.update(
            {
                f"packed{n}": vmem((2, 8, 32, piece), BF16),
                f"g_pair{n}": vmem((8, 32, piece), BF16),
                f"g_tx{n}": vmem((7, 32, piece), BF16),
                f"g_rx{n}": vmem((7, 32, piece), BF16),
                f"y_tx{n}": vmem((8, 4, piece), F32),
                f"y_rx{n}": vmem((7, 4, piece), F32),
                f"y_all{n}": vmem((8, 4, piece), F32),
                f"g_all{n}": vmem((2, 8, 32, piece), BF16),
                f"gp_sem{n}": dma(2),
                f"gc_sem{n}": dma(2, 7),
                f"gy1_sem{n}": dma(2, 7),
                f"gy2_sem{n}": dma(2, 7),
                f"ga_sem{n}": dma(2, 7),
                f"gf_sem{n}": dma(2, 8),
            }
        )
    return table


THINKER = dict(
    gate_w=pltpu.VMEM((2, HALF, 512), BF16),
    up_w=pltpu.VMEM((2, HALF, 512), BF16),
    down_w=pltpu.VMEM((2, HALF, 512), BF16),
    bridge_w=pltpu.VMEM((512, 3584), BF16),
    own_half=pltpu.VMEM((8, 16, 2 * HALF), F32),
    down_own=pltpu.VMEM((8, 16, 512), F32),
)
TALKER = dict(
    mixed=pltpu.VMEM((192, 3584), F32),
    normal=pltpu.VMEM((192, 3584), BF16),
    query=pltpu.VMEM((HEADS, 192, HD), BF16),
    score=pltpu.VMEM((336, 3072), F32),
    expo=pltpu.VMEM((336, 3072), BF16),
    attn_v=pltpu.VMEM((192, 1792), BF16),
    dvt=pltpu.VMEM((KVH, HD, 3072), F32),
    qgrad=pltpu.VMEM((192, 1792), BF16),
    p_aq=pltpu.VMEM((64, 3584), F32),
    p_av=pltpu.VMEM((64, 3584), F32),
    p_bq=pltpu.VMEM((64, 1792), F32),
    p_bv=pltpu.VMEM((64, 256), F32),
)


def weight_copy(r, kind, n):
    gx, gy, chip, core = place()
    z = gy // 2
    x_hi = gy % 2
    flip = 1 - x_hi
    up, down, far = (z + 1) % 4 * 2, (z + 3) % 4 * 2, (z + 2) % 4 * 2
    cross = ((chip + 1 - 2 * (chip % 2)) * 2 + core, z * 2 + flip)
    z_up, z_down = (gx, up + x_hi), (gx, down + x_hi)
    partner = (chip * 2 + 1 - core, gy)
    piece, part, peer = (
        (gy, None, cross),
        (gy, None, z_up),
        (gy, None, z_down),
        (z * 2 + flip, 0 if kind == "q" else None, z_up),
        (z * 2 + flip, 1 if kind == "q" else None, z_down),
        (down + x_hi, 0, z_up),
        (up + x_hi, 1, z_down),
        (down + flip, 0, z_up),
        (up + flip, 1, z_down),
        (z * 2 + flip, None, partner),
        (down + x_hi, None, partner),
        (up + x_hi, None, partner),
        (down + flip, None, partner),
        (up + flip, None, partner),
        (far + x_hi, None, partner),
        (far + flip, None, partner),
        (down + x_hi, 1, cross),
        (up + x_hi, 0, cross),
    )[n]
    cols = pl.ds(pl.multiple_of(core * 1792, 128), 1792)
    if kind == "q":
        rows = 224 if part is None else 112
        first = pl.multiple_of(piece * 224 + (0 if part is None else 112 * part), 16)
        ref, sem = r.all_q.at[pl.ds(first, rows), cols], r.wq_sem
    else:
        kinds = pl.ds(0, 2) if part is None else pl.ds(part, 1)
        rows = pl.ds(pl.multiple_of(piece * 32, 32), 32)
        ref, sem = r.all_kv.at[kinds, rows, cols], r.wkv_sem
    return remote(ref, ref, sem.at[0, n], sem.at[1, n], peer)


def weights_go(r, kind, *numbers):
    for n in numbers:
        weight_copy(r, kind, n).start()


def weights_wait(r, kind, *numbers):
    for n in numbers:
        weight_copy(r, kind, n).wait()


def early_loads(r):
    gy = lax.axis_index("gy")
    rows = pl.ds(pl.multiple_of(gy * 32, 32), 32)
    plan = [
        (r.wk, r.all_kv.at[0, rows]),
        (r.wv, r.all_kv.at[1, rows]),
        (r.wq, r.all_q.at[pl.ds(pl.multiple_of(gy * 224, 32), 224)]),
        (r.x, r.x_v),
        (r.resid, r.resid_v),
    ]
    return [pltpu.make_async_copy(a, b, r.load_sem.at[i]) for i, (a, b) in enumerate(plan)]


def late_loads(r):
    plan = [
        (r.stream, r.stream_v),
        (r.a_q, r.a_v_q),
        (r.a_v, r.a_v_v),
        (r.b_q, r.b_v_q),
        (r.b_v, r.b_v_v),
        (r.og, r.og_v),
    ]
    return [pltpu.make_async_copy(a, b, r.load_sem.at[5 + i]) for i, (a, b) in enumerate(plan)]


def think(r):
    gx, gy, chip, core = place()
    other = 1 - core
    partner = (chip * 2 + other, gy)
    chips = [((chip + k) % 8 * 2 + core, gy) for k in range(1, 8)]
    columns = [(gx, (gy + k) % 8) for k in range(1, 8)]
    row = [((gx + k) % 16, gy) for k in range(1, 16)]
    cross = ((chip + 1 - 2 * (chip % 2)) * 2 + core, gy + 1 - 2 * (gy % 2))

    first = early_loads(r)
    for copy in first:
        copy.start()
    plan = [
        (r.gate.at[pl.ds(0, HALF)], r.gate_w.at[0]),
        (r.gate.at[pl.ds(HALF, REST)], r.gate_w.at[1, pl.ds(0, REST)]),
        (r.up.at[pl.ds(0, HALF)], r.up_w.at[0]),
        (r.up.at[pl.ds(HALF, REST)], r.up_w.at[1, pl.ds(0, REST)]),
        (r.down.at[pl.ds(0, HALF)], r.down_w.at[0]),
        (r.down.at[pl.ds(HALF, REST)], r.down_w.at[1, pl.ds(0, REST)]),
        (r.bridge, r.bridge_w),
    ]
    loads = [pltpu.make_async_copy(a, b, r.load_sem.at[11 + i]) for i, (a, b) in enumerate(plan)]
    for copy in loads:
        copy.start()
    for copy in late_loads(r):
        copy.start()
    pad = jnp.zeros((HALF - REST, 512), BF16)
    r.gate_w[1, REST:] = pad
    r.up_w[1, REST:] = pad
    r.down_w[1, REST:] = pad

    greet(row + columns + [cross])

    first[0].wait()
    first[1].wait()
    weights_go(r, "kv", 0, 1, 2)
    first[2].wait()
    weights_go(r, "q", 0, 1, 2)

    first[3].wait()
    first[4].wait()
    for copy in loads[:4]:
        copy.wait()
    x = r.x_v[...]
    for half, is_own in ((other, False), (core, True)):
        for side, weight in ((0, r.gate_w), (1, r.up_w)):
            for c in range(HALF // CHUNK):
                part = dot_nt(x, weight[half, c * CHUNK : (c + 1) * CHUNK])
                part = part.reshape(8, 16, CHUNK)
                lo = side * HALF + c * CHUNK
                if is_own:
                    r.own_half[:, :, lo : lo + CHUNK] = part
                else:
                    r.pair_tx[:, :, lo : lo + CHUNK] = part.astype(BF16)
        if not is_own:
            pair_copy = send(r.pair_tx, r.pair_rx, r.pair_sem.at[0], r.pair_sem.at[1], partner)
    pair_copy.wait()

    chip_copies = []
    for k in range(1, 8):
        peer = (chip + k) % 8
        r.chip_tx[k - 1] = (r.own_half[peer] + r.pair_rx[peer].astype(F32)).astype(BF16)
        chip_copies.append(
            send(
                r.chip_tx.at[k - 1],
                r.chip_rx.at[k - 1],
                r.chip_sem.at[0, k - 1],
                r.chip_sem.at[1, k - 1],
                chips[k - 1],
            )
        )
    total = r.own_half[chip] + r.pair_rx[chip].astype(F32)
    for k in range(7):
        chip_copies[k].wait()
        total = total + r.chip_rx[k].astype(F32)
    gate = total[:, :HALF]
    r.hidden[core, chip] = (gate / (1.0 + jnp.exp(-gate)) * total[:, HALF:]).astype(BF16)

    fan_out(r.hidden, r.hid_sem, chip, core, chips)
    place_at = gx * 192 + lax.broadcasted_iota(jnp.int32, (192, 128), 0)
    angles = place_at.astype(F32) * r.freq[...]
    r.cos[...] = jnp.cos(angles)
    low_half = lax.broadcasted_iota(jnp.int32, (192, 128), 1) < 64
    r.sin[...] = jnp.sin(angles) * jnp.where(low_half, -1.0, 1.0)
    finish = relay_to_partner(r.hidden, r.hid_sem, r.hidf_sem, chip, core, chips, partner)
    loads[4].wait()
    loads[5].wait()
    finish()
    down = jnp.dot(r.hidden[0].reshape(128, HALF), r.down_w[0], preferred_element_type=F32)
    down = down + jnp.dot(
        r.hidden[1].reshape(128, HALF), r.down_w[1], preferred_element_type=F32
    )
    down = down.reshape(8, 16, 512)
    r.down_own[...] = down
    r.down_tx[...] = down.astype(BF16)
    gy_copies = [
        send(
            r.down_tx.at[(gy + k) % 8],
            r.down_rx.at[k - 1],
            r.gy_sem.at[0, k - 1],
            r.gy_sem.at[1, k - 1],
            columns[k - 1],
        )
        for k in range(1, 8)
    ]
    weights_wait(r, "kv", 0, 1, 2)
    weights_go(r, "kv", 3, 4, 5, 6, 9, 10, 11)
    loads[6].wait()
    tokens = r.down_own[gy] + r.resid_v[...].astype(F32)
    for k in range(7):
        gy_copies[k].wait()
        tokens = tokens + r.down_rx[k].astype(F32)
    weights_wait(r, "q", 0, 1, 2)
    weights_go(r, "q", 5, 6, 16, 17, 9, 10, 11)

    thinker_out = tokens.astype(BF16)
    for h in range(2):
        r.bridge_own[h] = jnp.dot(
            thinker_out, r.bridge_w[:, h * 1792 : (h + 1) * 1792], preferred_element_type=F32
        )
    send(r.bridge_own.at[other], r.bridge_rx, r.bp_sem.at[0], r.bp_sem.at[1], partner).wait()
    summed = r.bridge_own[core] + r.bridge_rx[...]
    r.bridge_tx[...] = summed.astype(BF16)
    b_copies = [
        send(r.bridge_tx, r.bridge_peers.at[k], r.bc_sem.at[0, k], r.bc_sem.at[1, k], chips[k])
        for k in range(7)
    ]
    weights_wait(r, "kv", 3, 4)
    weights_go(r, "kv", 7, 8, 12, 13)
    weights_go(r, "q", 3, 4)
    for k in range(7):
        b_copies[k].wait()
        summed = summed + r.bridge_peers[k].astype(F32)
    r.bridge_half[core] = summed.astype(BF16)
    send(
        r.bridge_half.at[core], r.bridge_half.at[core], r.bf_sem.at[0], r.bf_sem.at[1], partner
    ).wait()


def fan_out(ref, sem, chip, core, chips):
    here = ref.at[chip, core] if ref.shape[0] == 8 else ref.at[core, chip]
    for k in range(7):
        send(here, here, sem.at[0, k], sem.at[1, k], chips[k])


def relay_to_partner(ref, sem, fwd_sem, chip, core, chips, partner):
    def at(which):
        return ref.at[which, core] if ref.shape[0] == 8 else ref.at[core, which]

    here = at(chip)
    passed = [send(here, here, fwd_sem.at[0, 7], fwd_sem.at[1, 7], partner)]
    for k in range(7):
        remote(here, here, sem.at[0, k], sem.at[1, k], chips[k]).wait()
        block = at((chip + 7 - k) % 8)
        passed.append(send(block, block, fwd_sem.at[0, k], fwd_sem.at[1, k], partner))

    def finish():
        for copy in passed:
            copy.wait()

    return finish


def reduce_group(r, n, parts, outs):
    gx, gy, chip, core = place()
    other = 1 - core
    partner = (chip * 2 + other, gy)
    chips = [((chip + k) % 8 * 2 + core, gy) for k in range(1, 8)]
    columns = [(gx, (gy + k) % 8) for k in range(1, 8)]

    def own(name):
        return getattr(r, f"{name}{n}")

    packed, g_pair, g_tx, g_rx = own("packed"), own("g_pair"), own("g_tx"), own("g_rx")
    y_tx, y_rx, y_all, g_all = own("y_tx"), own("y_rx"), own("y_all"), own("g_all")
    for name, done, chunk, offset, size in segments(n):
        for h in range(2):
            if name is None:
                packed[h, chunk, :, offset : offset + size] = jnp.zeros((32, size), BF16)
            else:
                packed[h, chunk, :, offset : offset + size] = parts[name][
                    32 * h : 32 * h + 32, done : done + size
                ].astype(BF16)
    sem = own("gp_sem")
    pair = send(packed.at[other], g_pair, sem.at[0], sem.at[1], partner)
    yield
    pair.wait()
    sem = own("gc_sem")
    copies = []
    for k in range(1, 8):
        peer = (chip + k) % 8
        g_tx[k - 1] = (packed[core, peer].astype(F32) + g_pair[peer].astype(F32)).astype(BF16)
        copies.append(
            send(g_tx.at[k - 1], g_rx.at[k - 1], sem.at[0, k - 1], sem.at[1, k - 1], chips[k - 1])
        )
    total = packed[core, chip].astype(F32) + g_pair[chip].astype(F32)
    yield
    for k in range(7):
        copies[k].wait()
        total = total + g_rx[k].astype(F32)
    for i in range(8):
        y_tx[i] = total[4 * i : 4 * i + 4]
    sem = own("gy1_sem")
    copies = [
        send(
            y_tx.at[(gy + k) % 8], y_rx.at[k - 1], sem.at[0, k - 1], sem.at[1, k - 1], columns[k - 1]
        )
        for k in range(1, 8)
    ]
    total = y_tx[gy]
    yield
    for k in range(7):
        copies[k].wait()
        total = total + y_rx[k]
    y_all[gy] = total
    sem = own("gy2_sem")
    copies = [
        send(y_all.at[gy], y_all.at[gy], sem.at[0, k], sem.at[1, k], columns[k]) for k in range(7)
    ]
    yield
    for copy in copies:
        copy.wait()
    g_all[core, chip] = jnp.concatenate([y_all[i] for i in range(8)], axis=0).astype(BF16)
    fan_out(g_all, own("ga_sem"), chip, core, chips)
    yield
    finish = relay_to_partner(g_all, own("ga_sem"), own("gf_sem"), chip, core, chips, partner)
    yield
    finish()
    for name, done, chunk, offset, size in segments(n):
        if name is not None:
            for h in range(2):
                outs[name][32 * h : 32 * h + 32, done : done + size] = g_all[
                    h, chunk, :, offset : offset + size
                ].astype(F32)


def talk(r):
    gx, gy, chip, core = place()
    other = 1 - core
    partner = (chip * 2 + other, gy)
    chips = [((chip + k) % 8 * 2 + core, gy) for k in range(1, 8)]
    row = [((gx + k) % 16, gy) for k in range(1, 16)]
    kv = r.kv

    for copy in late_loads(r):
        copy.wait()
    picks = (r.index[...] == lax.broadcasted_iota(jnp.int32, (16, 192), 0)).astype(F32)
    picks = jnp.transpose(picks).astype(BF16)
    squares = jnp.zeros((192, HD), F32)
    for c in range(7):
        at = slice(512 * c, 512 * c + 512)
        pieces = []
        for lo, hi in ((512 * c, 512 * c + 256), (512 * c + 256, 512 * c + 512)):
            half, off = divmod(lo, 1792)
            pieces.append(r.bridge_half[half, :, off : off + 256])
        rows = jnp.concatenate(pieces, axis=1)
        mix = r.stream_v[:, at].astype(F32) + jnp.dot(picks, rows, preferred_element_type=F32)
        r.mixed[:, at] = mix
        for t in range(4):
            m = mix[:, t * HD : (t + 1) * HD]
            squares = squares + m * m
    rate = lax.rsqrt(jnp.sum(squares, axis=1, keepdims=True) / 3584.0 + norm_eps)
    for c in range(28):
        at = slice(128 * c, 128 * c + 128)
        r.normal[:, at] = (r.mixed[:, at] * rate * r.gain[c : c + 1]).astype(BF16)

    normal = r.normal[...]
    low_q = dot_nt(normal, r.a_v_q[...]).astype(BF16)
    low_v = dot_nt(normal, r.a_v_v[...]).astype(BF16)
    r.low[chip, core, :, :64] = low_q
    r.low[chip, core, :, 64:] = low_v
    weights_wait(r, "kv", 5, 6)
    weights_go(r, "kv", 14)
    weights_wait(r, "kv", 7, 8)
    weights_go(r, "kv", 15)
    weights_wait(r, "kv", *range(9, 16))
    keys = dot_nt(normal, r.all_kv[0])
    values = dot_nt(normal, r.all_kv[1]) + jnp.dot(
        low_v, r.b_v_v[...], preferred_element_type=F32
    )
    for g in range(KVH):
        head = keys[:, g * HD : (g + 1) * HD]
        kv[chip, core, :, g * HD : (g + 1) * HD] = (
            head * r.cos[...] + pltpu.roll(head, 64, 1) * r.sin[...]
        ).astype(BF16)
    kv[chip, core, :, 256:] = values.astype(BF16)
    fan_out(kv, r.kv_sem, chip, core, chips)
    fan_out(r.low, r.low_sem, chip, core, chips)
    r.dvt[...] = jnp.zeros_like(r.dvt)

    weights_wait(r, "q", 5, 6)
    weights_go(r, "q", 14)
    weights_wait(r, "q", 3, 4)
    weights_go(r, "q", 7, 8)
    weights_wait(r, "q", 16, 17)
    weights_go(r, "q", 12, 13)
    weights_wait(r, "q", 7, 8)
    weights_go(r, "q", 15)
    weights_wait(r, "q", *range(9, 16))

    def project(i, carry):
        at = pl.ds(pl.multiple_of(i * 256, 128), 256)
        pre = dot_nt(r.normal[...], r.all_q[at]) + jnp.dot(
            r.low[chip, core, :, :64], r.b_v_q[:, at], preferred_element_type=F32
        )
        for t in range(2):
            head = pre[:, t * HD : (t + 1) * HD]
            r.query[2 * i + t] = (
                head * r.cos[...] + pltpu.roll(head, 64, 1) * r.sin[...]
            ).astype(BF16)
        return carry

    lax.fori_loop(0, 7, project, 0)
    kv_finish = relay_to_partner(kv, r.kv_sem, r.kvf_sem, chip, core, chips, partner)
    low_finish = relay_to_partner(r.low, r.low_sem, r.lowf_sem, chip, core, chips, partner)
    kv_finish()

    scale = 1.0 / math.sqrt(HD)
    fold = scale * math.log2(math.e)
    span = 768

    def keys_at(group, j):
        at = pl.ds(pl.multiple_of(group * HD, 128), HD)
        return kv[2 * j : 2 * j + 2, :, :, at].reshape(span, HD)

    def values_at(group, j):
        at = pl.ds(pl.multiple_of(256 + group * HD, 128), HD)
        return kv[2 * j : 2 * j + 2, :, :, at].reshape(span, HD)

    block, rows = 48, 336

    def attend(b, carry):
        group = b // 4
        here = pl.ds(pl.multiple_of(b % 4 * block, 16), block)
        heads = [pl.ds(pl.multiple_of((group * 7 + i) * HD, 128), HD) for i in range(7)]

        def stacked(pieces):
            return jnp.concatenate(pieces, axis=0)

        q = r.query[pl.ds(group * 7, 7), here].reshape(rows, HD)
        first = gx * 192 + b % 4 * block
        place_at = first + lax.broadcasted_iota(jnp.int32, (block, 1), 0)
        lim = stacked([jnp.maximum(place_at, r.offset[0] - 1)] * 7)
        top = jnp.full((rows, HD), -jnp.inf, F32)
        for j in range(4):
            s = dot_nt(q, keys_at(group, j))
            spot = lax.broadcasted_iota(jnp.int32, (rows, span), 1) + j * span
            s = jnp.where(spot <= lim, s, -1e30)
            r.score[:, j * span : (j + 1) * span] = s
            for t in range(span // HD):
                top = jnp.maximum(top, s[:, t * HD : (t + 1) * HD])
        peak = jnp.max(top, axis=1, keepdims=True) * fold
        mass = jnp.zeros((rows, HD), F32)
        out = jnp.zeros((rows, HD), F32)
        for j in range(4):
            e = jnp.exp2(r.score[:, j * span : (j + 1) * span] * fold - peak)
            for t in range(span // HD):
                mass = mass + e[:, t * HD : (t + 1) * HD]
            e = e.astype(BF16)
            r.expo[:, j * span : (j + 1) * span] = e
            out = out + jnp.dot(e, values_at(group, j), preferred_element_type=F32)
        inverse = 1.0 / jnp.sum(mass, axis=1, keepdims=True)
        out = (out * inverse).astype(BF16)
        cot = stacked([r.og_v[here, at] for at in heads])
        wide = cot.astype(F32)
        inner = jnp.sum(wide * out.astype(F32), axis=1, keepdims=True)
        turned = jnp.transpose(wide * inverse).astype(BF16)
        dq = jnp.zeros((rows, HD), F32)
        for j in range(4):
            e = r.expo[:, j * span : (j + 1) * span]
            dp = dot_nt(cot, values_at(group, j))
            ds = (e.astype(F32) * (dp - inner)).astype(BF16)
            dq = dq + jnp.dot(ds, keys_at(group, j), preferred_element_type=F32)
            r.dvt[group, :, j * span : (j + 1) * span] += jnp.dot(
                turned, e, preferred_element_type=F32
            )
        dq = dq * (inverse * scale)
        for i, at in enumerate(heads):
            part = slice(block * i, block * i + block)
            r.attn_v[here, at] = out[part]
            piece = dq[part]
            r.qgrad[here, at] = (
                piece * r.cos[here] - pltpu.roll(piece, 64, 1) * r.sin[here]
            ).astype(BF16)
        return carry

    lax.fori_loop(0, 2 * 4, attend, 0)
    leaving = [pltpu.make_async_copy(r.attn_v, r.attn, r.out_sem.at[0])]
    leaving[0].start()

    for j in range(8):
        at = slice(384 * j, 384 * j + 384)
        part = jnp.dot(
            r.b_v_v[:, :HD], r.dvt[0, :, at].astype(BF16), preferred_element_type=F32
        ) + jnp.dot(r.b_v_v[:, HD:], r.dvt[1, :, at].astype(BF16), preferred_element_type=F32)
        r.dl_tx[2 * j] = part[:, :192].astype(BF16)
        r.dl_tx[2 * j + 1] = pltpu.roll(part, 192, 1)[:, :192].astype(BF16)
    dl_copies = [
        send(
            r.dl_tx.at[(gx + k) % 16],
            r.dl_rx.at[k - 1],
            r.dl_sem.at[0, k - 1],
            r.dl_sem.at[1, k - 1],
            row[k - 1],
        )
        for k in range(1, 16)
    ]
    low_finish()
    low_t = jnp.transpose(r.low[chip, core].astype(F32)).astype(BF16)
    r.p_bq[...] = jnp.dot(low_t[:64], r.qgrad[...], preferred_element_type=F32)
    dlow_q = dot_nt(r.b_v_q[...], r.qgrad[...]).astype(BF16)
    r.p_aq[...] = jnp.dot(dlow_q, r.normal[...], preferred_element_type=F32)
    for g in range(KVH):
        part = jnp.zeros((HD, HD), F32)
        for j in range(4):
            low = r.low[2 * j : 2 * j + 2].reshape(span, HD)
            part = part + jnp.dot(
                r.dvt[g, :, j * span : (j + 1) * span].astype(BF16),
                low,
                preferred_element_type=F32,
            )
        r.p_bv[:, g * HD : (g + 1) * HD] = jnp.transpose(part)[64:]
    parts = dict(aq=r.p_aq, av=r.p_av, bq=r.p_bq, bv=r.p_bv)
    outs = parts
    early = reduce_group(r, 0, parts, outs)
    next(early)
    next(early)
    dlow = r.dl_tx[gx].astype(F32)
    for k in range(15):
        dl_copies[k].wait()
        dlow = dlow + r.dl_rx[k].astype(F32)
    r.p_av[...] = jnp.dot(dlow.astype(BF16), r.normal[...], preferred_element_type=F32)
    late = reduce_group(r, 1, parts, outs)
    running = [late, early]
    while running:
        for group in list(running):
            if next(group, "end") == "end":
                running.remove(group)
                done = ("av",) if group is late else ("aq", "bq", "bv")
                for name in done:
                    copy = pltpu.make_async_copy(
                        parts[name], getattr(r, name), r.out_sem.at[len(leaving)]
                    )
                    copy.start()
                    leaving.append(copy)
    for copy in leaving:
        copy.wait()


def kernel(names, *refs):
    r = Box()
    for name, ref in zip(names, refs, strict=True):
        setattr(r, name, ref)

    def scoped(run, table):
        def inner(*more):
            box = Box()
            box.__dict__.update(r.__dict__)
            for name, ref in zip(table, more, strict=True):
                setattr(box, name, ref)
            run(box)

        pl.run_scoped(inner, *table.values())

    scoped(think, THINKER)
    scoped(talk, TALKER)


def whole(*args):
    vmem = pl.BlockSpec(memory_space=pltpu.VMEM)
    hbm = pl.BlockSpec(memory_space=pltpu.HBM)
    scratch = shared_scratch()
    names = INPUTS + OUTPUTS + list(scratch)
    return pl.pallas_call(
        functools.partial(kernel, names),
        out_shape=(
            jax.ShapeDtypeStruct((192, 1792), BF16),
            jax.ShapeDtypeStruct((64, 3584), F32),
            jax.ShapeDtypeStruct((64, 3584), F32),
            jax.ShapeDtypeStruct((64, 1792), F32),
            jax.ShapeDtypeStruct((64, 256), F32),
        ),
        in_specs=[hbm] * 15 + [vmem] * 3 + [pl.BlockSpec(memory_space=pltpu.SMEM)],
        out_specs=(hbm,) * 5,
        scratch_shapes=list(scratch.values()),
        compiler_params=pltpu.CompilerParams(
            collective_id=0, has_side_effects=True, vmem_limit_bytes=63 << 20
        ),
        name="layer",
    )(*args)


def on_device(
    thinker_normed,
    thinker_resid,
    gate_weight,
    up_weight,
    down_weight,
    bridge_weight,
    talker_stream,
    norm_gain,
    w_query,
    w_key,
    w_value,
    a_query,
    b_query,
    a_value,
    b_value,
    text_index,
    span_offset,
    out_grad,
):
    seq_count, rows_seq, columns = thinker_normed.shape
    angle = np.float32(rope_base) ** (-(2.0 * np.arange(HD // 2, dtype=np.float32)) / HD)
    attn_out, grad_aq, grad_av, grad_bq, grad_bv = whole(
        thinker_normed.reshape(seq_count * rows_seq, columns),
        thinker_resid[0],
        gate_weight.T,
        up_weight.T,
        down_weight,
        bridge_weight,
        w_query.T,
        w_key.T,
        w_value.T,
        talker_stream[0],
        out_grad[0],
        a_query.T,
        a_value.T,
        b_query,
        b_value,
        norm_gain.reshape(28, 128),
        text_index,
        jnp.asarray(np.concatenate([angle, angle])[None], F32),
        span_offset,
    )
    return (attn_out[None], grad_aq.T, grad_bq, grad_av.T, grad_bv)


def solution(mesh):
    return jax.shard_map(
        on_device,
        mesh=mesh,
        in_specs=(
            P(None, None, "gx"),
            P("gy", None, "gx"),
            P("gx", "gy"),
            P("gx", "gy"),
            P("gy", "gx"),
            P("gx", None),
            P("gy", "gx", None),
            P(),
            P(None, "gy"),
            P(None, "gy"),
            P(None, "gy"),
            P(),
            P(),
            P(),
            P(),
            P("gy", "gx"),
            P("gy"),
            P("gy", "gx", None),
        ),
        out_specs=(P("gy", "gx", None), P(), P(), P(), P()),
        check_vma=False,
    )
```

```python
import functools
import math

import jax
import jax.numpy as jnp
import numpy as np
from jax import lax
from jax.experimental import pallas as pl
from jax.experimental.pallas import tpu as pltpu
from jax.sharding import PartitionSpec as P

HEADS = 14
KVH = 2
HD = 128
MESH = pl.DeviceIdType.MESH
F32 = jnp.float32
BF16 = jnp.bfloat16

rope_base = 1000000.0
norm_eps = 1e-06


def place():
    gx = lax.axis_index("gx")
    gy = lax.axis_index("gy")
    return gx, gy, gx // 2, gx % 2


def greet(peers):
    barrier = pltpu.get_barrier_semaphore()
    for peer in peers:
        pl.semaphore_signal(barrier, inc=1, device_id=peer, device_id_type=MESH)
    pl.semaphore_wait(barrier, len(peers))


def remote(src, dst, send_sem, recv_sem, peer):
    return pltpu.make_async_remote_copy(
        src_ref=src,
        dst_ref=dst,
        send_sem=send_sem,
        recv_sem=recv_sem,
        device_id=peer,
        device_id_type=MESH,
    )


def send(*args):
    copy = remote(*args)
    copy.start()
    return copy


def dot_nt(a, b):
    return lax.dot_general(a, b, (((1,), (1,)), ((), ())), preferred_element_type=F32)


HALF = 1920
REST = 1776
CHUNK = 640
GROUPS = (
    (768, (("aq", 3584), ("bq", 1792), ("bv", 256))),
    (512, (("av", 3584),)),
)


def segments(group):
    piece, parts = GROUPS[group]
    start = 0
    for name, width in parts:
        done = 0
        while done < width:
            chunk, offset = divmod(start + done, piece)
            size = min(width - done, piece - offset)
            yield name, done, chunk, offset, size
            done += size
        start += width
    if start < 8 * piece:
        chunk, offset = divmod(start, piece)
        while chunk < 8:
            yield None, 0, chunk, offset, piece - offset
            chunk, offset = chunk + 1, 0


class Box:
    pass


INPUTS = [
    "x", "resid", "gate", "up", "down", "bridge", "wq", "wk", "wv", "stream", "og", "a_q",
    "a_v", "b_q", "b_v", "gain", "index", "freq", "offset",
]
OUTPUTS = ["attn", "aq", "av", "bq", "bv"]


def dma(*shape):
    return pltpu.SemaphoreType.DMA(shape)


def shared_scratch():
    vmem = pltpu.VMEM
    table = dict(
        all_q=vmem((1792, 3584), BF16),
        all_kv=vmem((2, 256, 3584), BF16),
        cos=vmem((192, 128), F32),
        sin=vmem((192, 128), F32),
        x_v=vmem((128, 512), BF16),
        resid_v=vmem((16, 512), BF16),
        stream_v=vmem((192, 3584), BF16),
        og_v=vmem((192, 1792), BF16),
        a_v_q=vmem((64, 3584), BF16),
        a_v_v=vmem((64, 3584), BF16),
        b_v_q=vmem((64, 1792), BF16),
        b_v_v=vmem((64, 256), BF16),
        pair_tx=vmem((8, 16, 2 * HALF), BF16),
        pair_rx=vmem((8, 16, 2 * HALF), BF16),
        chip_tx=vmem((7, 16, 2 * HALF), BF16),
        chip_rx=vmem((7, 16, 2 * HALF), BF16),
        hidden=vmem((2, 8, 16, HALF), BF16),
        down_tx=vmem((8, 16, 512), BF16),
        down_rx=vmem((7, 16, 512), BF16),
        bridge_own=vmem((2, 16, 1792), F32),
        bridge_rx=vmem((16, 1792), F32),
        bridge_tx=vmem((16, 1792), BF16),
        bridge_peers=vmem((7, 16, 1792), BF16),
        bridge_half=vmem((2, 16, 1792), BF16),
        kv=vmem((8, 2, 192, 512), BF16),
        low=vmem((8, 2, 192, 128), BF16),
        normal=vmem((2, 192, 3584), BF16),
        dl_tx=vmem((16, 32, 384), BF16),
        dl_rx=vmem((15, 32, 384), BF16),
        norm_sem=dma(2),
        load_sem=dma(18),
        pair_sem=dma(2),
        chip_sem=dma(2, 7),
        hid_sem=dma(2, 7),
        hidf_sem=dma(2, 8),
        gy_sem=dma(2, 7),
        bp_sem=dma(2),
        bc_sem=dma(2, 7),
        bf_sem=dma(2),
        wq_sem=dma(2, 18),
        wkv_sem=dma(2, 16),
        kv_sem=dma(2, 7),
        kvf_sem=dma(2, 8),
        low_sem=dma(2, 7),
        lowf_sem=dma(2, 8),
        dl_sem=dma(2, 15),
        out_sem=dma(5),
    )
    for n, (piece, _) in enumerate(GROUPS):
        table.update(
            {
                f"packed{n}": vmem((2, 8, 32, piece), BF16),
                f"g_pair{n}": vmem((8, 32, piece), BF16),
                f"g_tx{n}": vmem((7, 32, piece), BF16),
                f"g_rx{n}": vmem((7, 32, piece), BF16),
                f"y_tx{n}": vmem((8, 4, piece), F32),
                f"y_rx{n}": vmem((7, 4, piece), F32),
                f"y_all{n}": vmem((8, 4, piece), F32),
                f"g_all{n}": vmem((2, 8, 32, piece), BF16),
                f"gp_sem{n}": dma(2),
                f"gc_sem{n}": dma(2, 7),
                f"gy1_sem{n}": dma(2, 7),
                f"gy2_sem{n}": dma(2, 7),
                f"ga_sem{n}": dma(2, 7),
                f"gf_sem{n}": dma(2, 8),
            }
        )
    return table


THINKER = dict(
    gate_w=pltpu.VMEM((2, HALF, 512), BF16),
    up_w=pltpu.VMEM((2, HALF, 512), BF16),
    down_w=pltpu.VMEM((2, HALF, 512), BF16),
    bridge_w=pltpu.VMEM((512, 3584), BF16),
    own_half=pltpu.VMEM((8, 16, 2 * HALF), F32),
    down_own=pltpu.VMEM((8, 16, 512), F32),
)
TALKER = dict(
    mixed=pltpu.VMEM((192, 3584), F32),
    query=pltpu.VMEM((HEADS, 192, HD), BF16),
    score=pltpu.VMEM((336, 3072), F32),
    bias=pltpu.VMEM((48, 3072), F32),
    expo=pltpu.VMEM((336, 3072), BF16),
    attn_v=pltpu.VMEM((192, 1792), BF16),
    dvt=pltpu.VMEM((KVH, HD, 3072), F32),
    qgrad=pltpu.VMEM((192, 1792), BF16),
    p_aq=pltpu.VMEM((64, 3584), F32),
    p_av=pltpu.VMEM((32, 3584), F32),
    p_bq=pltpu.VMEM((64, 1792), F32),
    p_bv=pltpu.VMEM((64, 256), F32),
    o_aq=pltpu.VMEM((64, 3584), BF16),
    o_av=pltpu.VMEM((64, 3584), BF16),
    o_bq=pltpu.VMEM((64, 1792), BF16),
    o_bv=pltpu.VMEM((64, 256), BF16),
)


def weight_copy(r, kind, n):
    gx, gy, chip, core = place()
    z = gy // 2
    x_hi = gy % 2
    flip = 1 - x_hi
    up, down, far = (z + 1) % 4 * 2, (z + 3) % 4 * 2, (z + 2) % 4 * 2
    cross = ((chip + 1 - 2 * (chip % 2)) * 2 + core, z * 2 + flip)
    z_up, z_down = (gx, up + x_hi), (gx, down + x_hi)
    partner = (chip * 2 + 1 - core, gy)
    piece, part, peer = (
        (gy, None, cross),
        (gy, None, z_up),
        (gy, None, z_down),
        (z * 2 + flip, 0 if kind == "q" else None, z_up),
        (z * 2 + flip, 1 if kind == "q" else None, z_down),
        (down + x_hi, 0, z_up),
        (up + x_hi, 1, z_down),
        (down + flip, 0, z_up),
        (up + flip, 1, z_down),
        (z * 2 + flip, None, partner),
        (down + x_hi, None, partner),
        (up + x_hi, None, partner),
        (down + flip, None, partner),
        (up + flip, None, partner),
        (far + x_hi, None, partner),
        (far + flip, None, partner),
        (down + x_hi, 1, cross),
        (up + x_hi, 0, cross),
    )[n]
    cols = pl.ds(pl.multiple_of(core * 1792, 128), 1792)
    if kind == "q":
        rows = 224 if part is None else 112
        first = pl.multiple_of(piece * 224 + (0 if part is None else 112 * part), 16)
        ref, sem = r.all_q.at[pl.ds(first, rows), cols], r.wq_sem
    else:
        kinds = pl.ds(0, 2) if part is None else pl.ds(part, 1)
        rows = pl.ds(pl.multiple_of(piece * 32, 32), 32)
        ref, sem = r.all_kv.at[kinds, rows, cols], r.wkv_sem
    return remote(ref, ref, sem.at[0, n], sem.at[1, n], peer)


def weights_go(r, kind, *numbers):
    for n in numbers:
        weight_copy(r, kind, n).start()


def weights_wait(r, kind, *numbers):
    for n in numbers:
        weight_copy(r, kind, n).wait()


def early_loads(r):
    gy = lax.axis_index("gy")
    rows = pl.ds(pl.multiple_of(gy * 32, 32), 32)
    plan = [
        (r.wk, r.all_kv.at[0, rows]),
        (r.wv, r.all_kv.at[1, rows]),
        (r.wq, r.all_q.at[pl.ds(pl.multiple_of(gy * 224, 32), 224)]),
        (r.x, r.x_v),
        (r.resid, r.resid_v),
    ]
    return [pltpu.make_async_copy(a, b, r.load_sem.at[i]) for i, (a, b) in enumerate(plan)]


def late_loads(r):
    plan = [
        (r.stream, r.stream_v),
        (r.a_q, r.a_v_q),
        (r.a_v, r.a_v_v),
        (r.b_q, r.b_v_q),
        (r.b_v, r.b_v_v),
        (r.og, r.og_v),
    ]
    return [pltpu.make_async_copy(a, b, r.load_sem.at[5 + i]) for i, (a, b) in enumerate(plan)]


def think(r):
    gx, gy, chip, core = place()
    other = 1 - core
    partner = (chip * 2 + other, gy)
    chips = [((chip + k) % 8 * 2 + core, gy) for k in range(1, 8)]
    columns = [(gx, (gy + k) % 8) for k in range(1, 8)]
    row = [((gx + k) % 16, gy) for k in range(1, 16)]
    cross = ((chip + 1 - 2 * (chip % 2)) * 2 + core, gy + 1 - 2 * (gy % 2))

    first = early_loads(r)
    for copy in first:
        copy.start()
    plan = [
        (r.gate.at[pl.ds(0, HALF)], r.gate_w.at[0]),
        (r.gate.at[pl.ds(HALF, REST)], r.gate_w.at[1, pl.ds(0, REST)]),
        (r.up.at[pl.ds(0, HALF)], r.up_w.at[0]),
        (r.up.at[pl.ds(HALF, REST)], r.up_w.at[1, pl.ds(0, REST)]),
        (r.down.at[pl.ds(0, HALF)], r.down_w.at[0]),
        (r.down.at[pl.ds(HALF, REST)], r.down_w.at[1, pl.ds(0, REST)]),
        (r.bridge, r.bridge_w),
    ]
    loads = [pltpu.make_async_copy(a, b, r.load_sem.at[11 + i]) for i, (a, b) in enumerate(plan)]
    for copy in loads:
        copy.start()
    for copy in late_loads(r):
        copy.start()
    pad = jnp.zeros((HALF - REST, 512), BF16)
    r.gate_w[1, REST:] = pad
    r.up_w[1, REST:] = pad
    r.down_w[1, REST:] = pad

    greet(row + columns + [cross])

    first[0].wait()
    first[1].wait()
    weights_go(r, "kv", 0, 1, 2)
    first[2].wait()
    weights_go(r, "q", 0, 1, 2)

    first[3].wait()
    first[4].wait()
    for copy in loads[:4]:
        copy.wait()
    x = r.x_v[...]
    for half, is_own in ((other, False), (core, True)):
        for side, weight in ((0, r.gate_w), (1, r.up_w)):
            for c in range(HALF // CHUNK):
                part = dot_nt(x, weight[half, c * CHUNK : (c + 1) * CHUNK])
                part = part.reshape(8, 16, CHUNK)
                lo = side * HALF + c * CHUNK
                if is_own:
                    r.own_half[:, :, lo : lo + CHUNK] = part
                else:
                    r.pair_tx[:, :, lo : lo + CHUNK] = part.astype(BF16)
        if not is_own:
            pair_copy = send(r.pair_tx, r.pair_rx, r.pair_sem.at[0], r.pair_sem.at[1], partner)
    pair_copy.wait()

    chip_copies = []
    for k in range(1, 8):
        peer = (chip + k) % 8
        r.chip_tx[k - 1] = (r.own_half[peer] + r.pair_rx[peer].astype(F32)).astype(BF16)
        chip_copies.append(
            send(
                r.chip_tx.at[k - 1],
                r.chip_rx.at[k - 1],
                r.chip_sem.at[0, k - 1],
                r.chip_sem.at[1, k - 1],
                chips[k - 1],
            )
        )
    total = r.own_half[chip] + r.pair_rx[chip].astype(F32)
    for k in range(7):
        chip_copies[k].wait()
        total = total + r.chip_rx[k].astype(F32)
    gate = total[:, :HALF]
    r.hidden[core, chip] = (gate / (1.0 + jnp.exp(-gate)) * total[:, HALF:]).astype(BF16)

    fan_out(r.hidden, r.hid_sem, chip, core, chips)
    place_at = gx * 192 + lax.broadcasted_iota(jnp.int32, (192, 128), 0)
    angles = place_at.astype(F32) * r.freq[...]
    r.cos[...] = jnp.cos(angles)
    low_half = lax.broadcasted_iota(jnp.int32, (192, 128), 1) < 64
    r.sin[...] = jnp.sin(angles) * jnp.where(low_half, -1.0, 1.0)
    finish = relay_to_partner(r.hidden, r.hid_sem, r.hidf_sem, chip, core, chips, partner)
    loads[4].wait()
    loads[5].wait()
    finish()
    down = jnp.dot(r.hidden[0].reshape(128, HALF), r.down_w[0], preferred_element_type=F32)
    down = down + jnp.dot(
        r.hidden[1].reshape(128, HALF), r.down_w[1], preferred_element_type=F32
    )
    down = down.reshape(8, 16, 512)
    r.down_own[...] = down
    r.down_tx[...] = down.astype(BF16)
    gy_copies = [
        send(
            r.down_tx.at[(gy + k) % 8],
            r.down_rx.at[k - 1],
            r.gy_sem.at[0, k - 1],
            r.gy_sem.at[1, k - 1],
            columns[k - 1],
        )
        for k in range(1, 8)
    ]
    weights_wait(r, "kv", 0, 1, 2)
    weights_go(r, "kv", 3, 4, 5, 6, 9, 10, 11)
    loads[6].wait()
    tokens = r.down_own[gy] + r.resid_v[...].astype(F32)
    for k in range(7):
        gy_copies[k].wait()
        tokens = tokens + r.down_rx[k].astype(F32)
    weights_wait(r, "q", 0, 1, 2)
    weights_go(r, "q", 5, 6, 16, 17, 9, 10, 11)

    thinker_out = tokens.astype(BF16)
    for h in range(2):
        r.bridge_own[h] = jnp.dot(
            thinker_out, r.bridge_w[:, h * 1792 : (h + 1) * 1792], preferred_element_type=F32
        )
    send(r.bridge_own.at[other], r.bridge_rx, r.bp_sem.at[0], r.bp_sem.at[1], partner).wait()
    summed = r.bridge_own[core] + r.bridge_rx[...]
    r.bridge_tx[...] = summed.astype(BF16)
    b_copies = [
        send(r.bridge_tx, r.bridge_peers.at[k], r.bc_sem.at[0, k], r.bc_sem.at[1, k], chips[k])
        for k in range(7)
    ]
    weights_wait(r, "kv", 3, 4)
    weights_go(r, "kv", 7, 8, 12, 13)
    weights_go(r, "q", 3, 4)
    for k in range(7):
        b_copies[k].wait()
        summed = summed + r.bridge_peers[k].astype(F32)
    r.bridge_half[core] = summed.astype(BF16)
    send(
        r.bridge_half.at[core], r.bridge_half.at[core], r.bf_sem.at[0], r.bf_sem.at[1], partner
    ).wait()


def fan_out(ref, sem, chip, core, chips):
    here = ref.at[chip, core] if ref.shape[0] == 8 else ref.at[core, chip]
    for k in range(7):
        send(here, here, sem.at[0, k], sem.at[1, k], chips[k])


def relay_to_partner(ref, sem, fwd_sem, chip, core, chips, partner):
    def at(which):
        return ref.at[which, core] if ref.shape[0] == 8 else ref.at[core, which]

    here = at(chip)
    passed = [send(here, here, fwd_sem.at[0, 7], fwd_sem.at[1, 7], partner)]
    for k in range(7):
        remote(here, here, sem.at[0, k], sem.at[1, k], chips[k]).wait()
        block = at((chip + 7 - k) % 8)
        passed.append(send(block, block, fwd_sem.at[0, k], fwd_sem.at[1, k], partner))

    def finish():
        for copy in passed:
            copy.wait()

    return finish


def reduce_group(r, n, parts, outs):
    gx, gy, chip, core = place()
    other = 1 - core
    partner = (chip * 2 + other, gy)
    chips = [((chip + k) % 8 * 2 + core, gy) for k in range(1, 8)]
    columns = [(gx, (gy + k) % 8) for k in range(1, 8)]

    def own(name):
        return getattr(r, f"{name}{n}")

    packed, g_pair, g_tx, g_rx = own("packed"), own("g_pair"), own("g_tx"), own("g_rx")
    y_tx, y_rx, y_all, g_all = own("y_tx"), own("y_rx"), own("y_all"), own("g_all")
    paired = n == 0
    for name, done, chunk, offset, size in segments(n):
        if not paired:
            value = jnp.zeros((32, size), F32) if name is None else parts[name][:, done : done + size]
            packed[core, chunk, :, offset : offset + size] = value.astype(BF16)
            continue
        for h in range(2):
            if name is None:
                packed[h, chunk, :, offset : offset + size] = jnp.zeros((32, size), BF16)
            else:
                packed[h, chunk, :, offset : offset + size] = parts[name][
                    32 * h : 32 * h + 32, done : done + size
                ].astype(BF16)
    if paired:
        sem = own("gp_sem")
        pair = send(packed.at[other], g_pair, sem.at[0], sem.at[1], partner)
        yield
        pair.wait()
    sem = own("gc_sem")
    copies = []
    for k in range(1, 8):
        peer = (chip + k) % 8
        block = packed.at[core, peer]
        if paired:
            block = g_tx.at[k - 1]
            block[...] = (packed[core, peer].astype(F32) + g_pair[peer].astype(F32)).astype(BF16)
        copies.append(
            send(block, g_rx.at[k - 1], sem.at[0, k - 1], sem.at[1, k - 1], chips[k - 1])
        )
    total = packed[core, chip].astype(F32)
    if paired:
        total = total + g_pair[chip].astype(F32)
    yield
    for k in range(7):
        copies[k].wait()
        total = total + g_rx[k].astype(F32)
    for i in range(8):
        y_tx[i] = total[4 * i : 4 * i + 4]
    sem = own("gy1_sem")
    copies = [
        send(
            y_tx.at[(gy + k) % 8], y_rx.at[k - 1], sem.at[0, k - 1], sem.at[1, k - 1], columns[k - 1]
        )
        for k in range(1, 8)
    ]
    total = y_tx[gy]
    yield
    for k in range(7):
        copies[k].wait()
        total = total + y_rx[k]
    y_all[gy] = total
    sem = own("gy2_sem")
    copies = [
        send(y_all.at[gy], y_all.at[gy], sem.at[0, k], sem.at[1, k], columns[k]) for k in range(7)
    ]
    yield
    for copy in copies:
        copy.wait()
    g_all[core, chip] = jnp.concatenate([y_all[i] for i in range(8)], axis=0).astype(BF16)
    fan_out(g_all, own("ga_sem"), chip, core, chips)
    yield
    finish = relay_to_partner(g_all, own("ga_sem"), own("gf_sem"), chip, core, chips, partner)
    yield
    finish()
    for name, done, chunk, offset, size in segments(n):
        if name is not None:
            for h in range(2):
                outs[name][32 * h : 32 * h + 32, done : done + size] = g_all[
                    h, chunk, :, offset : offset + size
                ]


def talk(r):
    gx, gy, chip, core = place()
    other = 1 - core
    partner = (chip * 2 + other, gy)
    chips = [((chip + k) % 8 * 2 + core, gy) for k in range(1, 8)]
    row = [((gx + k) % 16, gy) for k in range(1, 16)]
    kv = r.kv

    for copy in late_loads(r):
        copy.wait()
    picks = (r.index[...] == lax.broadcasted_iota(jnp.int32, (16, 192), 0)).astype(F32)
    picks = jnp.transpose(picks).astype(BF16)
    squares = jnp.zeros((192, HD), F32)
    for c in range(7):
        at = slice(512 * c, 512 * c + 512)
        pieces = []
        for lo, hi in ((512 * c, 512 * c + 256), (512 * c + 256, 512 * c + 512)):
            half, off = divmod(lo, 1792)
            pieces.append(r.bridge_half[half, :, off : off + 256])
        rows = jnp.concatenate(pieces, axis=1)
        mix = r.stream_v[:, at].astype(F32) + jnp.dot(picks, rows, preferred_element_type=F32)
        r.mixed[:, at] = mix
        for t in range(4):
            m = mix[:, t * HD : (t + 1) * HD]
            squares = squares + m * m
    rate = lax.rsqrt(jnp.sum(squares, axis=1, keepdims=True) / 3584.0 + norm_eps)
    for c in range(28):
        at = slice(128 * c, 128 * c + 128)
        r.normal[core, :, at] = (r.mixed[:, at] * rate * r.gain[c : c + 1]).astype(BF16)

    normal = r.normal[core]
    low_q = dot_nt(normal, r.a_v_q[...]).astype(BF16)
    low_v = dot_nt(normal, r.a_v_v[...]).astype(BF16)
    r.low[chip, core, :, :64] = low_q
    r.low[chip, core, :, 64:] = low_v
    weights_wait(r, "kv", 5, 6)
    weights_go(r, "kv", 14)
    weights_wait(r, "kv", 7, 8)
    weights_go(r, "kv", 15)
    weights_wait(r, "kv", *range(9, 16))
    keys = dot_nt(normal, r.all_kv[0])
    values = dot_nt(normal, r.all_kv[1]) + jnp.dot(
        low_v, r.b_v_v[...], preferred_element_type=F32
    )
    for g in range(KVH):
        head = keys[:, g * HD : (g + 1) * HD]
        kv[chip, core, :, g * HD : (g + 1) * HD] = (
            head * r.cos[...] + pltpu.roll(head, 64, 1) * r.sin[...]
        ).astype(BF16)
    kv[chip, core, :, 256:] = values.astype(BF16)
    fan_out(kv, r.kv_sem, chip, core, chips)
    fan_out(r.low, r.low_sem, chip, core, chips)
    here = r.normal.at[core]
    norm_copy = send(here, here, r.norm_sem.at[0], r.norm_sem.at[1], partner)
    r.dvt[...] = jnp.zeros_like(r.dvt)

    weights_wait(r, "q", 5, 6)
    weights_go(r, "q", 14)
    weights_wait(r, "q", 3, 4)
    weights_go(r, "q", 7, 8)
    weights_wait(r, "q", 16, 17)
    weights_go(r, "q", 12, 13)
    weights_wait(r, "q", 7, 8)
    weights_go(r, "q", 15)
    weights_wait(r, "q", *range(9, 16))

    scale = 1.0 / math.sqrt(HD)
    fold = scale * math.log2(math.e)

    def project(i, carry):
        at = pl.ds(pl.multiple_of(i * 256, 128), 256)
        pre = dot_nt(r.normal[core], r.all_q[at]) + jnp.dot(
            r.low[chip, core, :, :64], r.b_v_q[:, at], preferred_element_type=F32
        )
        for t in range(2):
            head = pre[:, t * HD : (t + 1) * HD]
            turned = head * r.cos[...] + pltpu.roll(head, 64, 1) * r.sin[...]
            r.query[2 * i + t] = (turned * fold).astype(BF16)
        return carry

    lax.fori_loop(0, 7, project, 0)
    kv_finish = relay_to_partner(kv, r.kv_sem, r.kvf_sem, chip, core, chips, partner)
    low_finish = relay_to_partner(r.low, r.low_sem, r.lowf_sem, chip, core, chips, partner)
    kv_finish()

    span = 768

    def keys_at(group, j):
        at = pl.ds(pl.multiple_of(group * HD, 128), HD)
        return kv[2 * j : 2 * j + 2, :, :, at].reshape(span, HD)

    def values_at(group, j):
        at = pl.ds(pl.multiple_of(256 + group * HD, 128), HD)
        return kv[2 * j : 2 * j + 2, :, :, at].reshape(span, HD)

    block, rows = 48, 336

    def attend(b, carry):
        group = b // 4
        here = pl.ds(pl.multiple_of(b % 4 * block, 16), block)
        heads = [pl.ds(pl.multiple_of((group * 7 + i) * HD, 128), HD) for i in range(7)]

        def stacked(pieces):
            return jnp.concatenate(pieces, axis=0)

        q = r.query[pl.ds(group * 7, 7), here].reshape(rows, HD)
        first = gx * 192 + b % 4 * block
        place_at = first + lax.broadcasted_iota(jnp.int32, (block, 1), 0)
        lim = jnp.maximum(place_at, r.offset[0] - 1)
        for j in range(4):
            spot = lax.broadcasted_iota(jnp.int32, (block, span), 1) + j * span
            r.bias[:, j * span : (j + 1) * span] = jnp.where(spot <= lim, 0.0, -1e30)
        top = jnp.full((rows, HD), -jnp.inf, F32)
        for j in range(4):
            s = dot_nt(q, keys_at(group, j)).reshape(7, block, span)
            s = (s + r.bias[:, j * span : (j + 1) * span][None]).reshape(rows, span)
            r.score[:, j * span : (j + 1) * span] = s
            for t in range(span // HD):
                top = jnp.maximum(top, s[:, t * HD : (t + 1) * HD])
        peak = jnp.max(top, axis=1, keepdims=True)
        mass = jnp.zeros((rows, HD), F32)
        out = jnp.zeros((rows, HD), F32)
        for j in range(4):
            e = jnp.exp2(r.score[:, j * span : (j + 1) * span] - peak)
            for t in range(span // HD):
                mass = mass + e[:, t * HD : (t + 1) * HD]
            e = e.astype(BF16)
            r.expo[:, j * span : (j + 1) * span] = e
            out = out + jnp.dot(e, values_at(group, j), preferred_element_type=F32)
        inverse = 1.0 / jnp.sum(mass, axis=1, keepdims=True)
        out = (out * inverse).astype(BF16)
        cot = stacked([r.og_v[here, at] for at in heads])
        wide = cot.astype(F32)
        inner = jnp.sum(wide * out.astype(F32), axis=1, keepdims=True)
        turned = jnp.transpose(wide * inverse).astype(BF16)
        dq = jnp.zeros((rows, HD), F32)
        for j in range(4):
            e = r.expo[:, j * span : (j + 1) * span]
            ds = (dot_nt(cot, values_at(group, j)) - inner).astype(BF16) * e
            dq = dq + jnp.dot(ds, keys_at(group, j), preferred_element_type=F32)
            r.dvt[group, :, j * span : (j + 1) * span] += jnp.dot(
                turned, e, preferred_element_type=F32
            )
        dq = dq * (inverse * scale)
        for i, at in enumerate(heads):
            part = slice(block * i, block * i + block)
            r.attn_v[here, at] = out[part]
            piece = dq[part]
            r.qgrad[here, at] = (
                piece * r.cos[here] - pltpu.roll(piece, 64, 1) * r.sin[here]
            ).astype(BF16)
        return carry

    lax.fori_loop(0, 2 * 4, attend, 0)
    leaving = [pltpu.make_async_copy(r.attn_v, r.attn, r.out_sem.at[0])]
    leaving[0].start()

    for j in range(8):
        at = slice(384 * j, 384 * j + 384)
        part = jnp.dot(
            r.b_v_v[:, :HD], r.dvt[0, :, at].astype(BF16), preferred_element_type=F32
        ) + jnp.dot(r.b_v_v[:, HD:], r.dvt[1, :, at].astype(BF16), preferred_element_type=F32)
        r.dl_tx[2 * j] = part[:32].astype(BF16)
        r.dl_tx[2 * j + 1] = part[32:].astype(BF16)
    dl_copies = [
        send(
            r.dl_tx.at[(gx + k) % 16],
            r.dl_rx.at[k - 1],
            r.dl_sem.at[0, k - 1],
            r.dl_sem.at[1, k - 1],
            row[k - 1],
        )
        for k in range(1, 16)
    ]
    low_finish()
    low_t = jnp.transpose(r.low[chip, core].astype(F32)).astype(BF16)
    r.p_bq[...] = jnp.dot(low_t[:64], r.qgrad[...], preferred_element_type=F32)
    dlow_q = dot_nt(r.b_v_q[...], r.qgrad[...]).astype(BF16)
    r.p_aq[...] = jnp.dot(dlow_q, r.normal[core], preferred_element_type=F32)
    for g in range(KVH):
        part = jnp.zeros((HD, HD), F32)
        for j in range(4):
            low = r.low[2 * j : 2 * j + 2].reshape(span, HD)
            part = part + jnp.dot(
                r.dvt[g, :, j * span : (j + 1) * span].astype(BF16),
                low,
                preferred_element_type=F32,
            )
        r.p_bv[:, g * HD : (g + 1) * HD] = jnp.transpose(part)[64:]
    parts = dict(aq=r.p_aq, av=r.p_av, bq=r.p_bq, bv=r.p_bv)
    outs = dict(aq=r.o_aq, av=r.o_av, bq=r.o_bq, bv=r.o_bv)
    early = reduce_group(r, 0, parts, outs)
    next(early)
    next(early)
    dlow = r.dl_tx[gx].astype(F32)
    for k in range(15):
        dl_copies[k].wait()
        dlow = dlow + r.dl_rx[k].astype(F32)
    norm_copy.wait()
    both = r.normal[...].reshape(384, 3584)
    r.p_av[...] = jnp.dot(dlow.astype(BF16), both, preferred_element_type=F32)
    late = reduce_group(r, 1, parts, outs)
    running = [late, early]
    while running:
        for group in list(running):
            if next(group, "end") == "end":
                running.remove(group)
                done = ("av",) if group is late else ("aq", "bq", "bv")
                for name in done:
                    copy = pltpu.make_async_copy(
                        outs[name], getattr(r, name), r.out_sem.at[len(leaving)]
                    )
                    copy.start()
                    leaving.append(copy)
    for copy in leaving:
        copy.wait()


def kernel(names, *refs):
    r = Box()
    for name, ref in zip(names, refs, strict=True):
        setattr(r, name, ref)

    def scoped(run, table):
        def inner(*more):
            box = Box()
            box.__dict__.update(r.__dict__)
            for name, ref in zip(table, more, strict=True):
                setattr(box, name, ref)
            run(box)

        pl.run_scoped(inner, *table.values())

    scoped(think, THINKER)
    scoped(talk, TALKER)


def whole(*args):
    vmem = pl.BlockSpec(memory_space=pltpu.VMEM)
    hbm = pl.BlockSpec(memory_space=pltpu.HBM)
    scratch = shared_scratch()
    names = INPUTS + OUTPUTS + list(scratch)
    return pl.pallas_call(
        functools.partial(kernel, names),
        out_shape=(
            jax.ShapeDtypeStruct((192, 1792), BF16),
            jax.ShapeDtypeStruct((64, 3584), BF16),
            jax.ShapeDtypeStruct((64, 3584), BF16),
            jax.ShapeDtypeStruct((64, 1792), BF16),
            jax.ShapeDtypeStruct((64, 256), BF16),
        ),
        in_specs=[hbm] * 15 + [vmem] * 3 + [pl.BlockSpec(memory_space=pltpu.SMEM)],
        out_specs=(hbm,) * 5,
        scratch_shapes=list(scratch.values()),
        compiler_params=pltpu.CompilerParams(
            collective_id=0, has_side_effects=True, vmem_limit_bytes=63 << 20
        ),
        name="layer",
    )(*args)


def on_device(
    thinker_normed,
    thinker_resid,
    gate_weight,
    up_weight,
    down_weight,
    bridge_weight,
    talker_stream,
    norm_gain,
    w_query,
    w_key,
    w_value,
    a_query,
    b_query,
    a_value,
    b_value,
    text_index,
    span_offset,
    out_grad,
):
    seq_count, rows_seq, columns = thinker_normed.shape
    angle = np.float32(rope_base) ** (-(2.0 * np.arange(HD // 2, dtype=np.float32)) / HD)
    attn_out, grad_aq, grad_av, grad_bq, grad_bv = whole(
        thinker_normed.reshape(seq_count * rows_seq, columns),
        thinker_resid[0],
        gate_weight.T,
        up_weight.T,
        down_weight,
        bridge_weight,
        w_query.T,
        w_key.T,
        w_value.T,
        talker_stream[0],
        out_grad[0],
        a_query.T,
        a_value.T,
        b_query,
        b_value,
        norm_gain.reshape(28, 128),
        text_index,
        jnp.asarray(np.concatenate([angle, angle])[None], F32),
        span_offset,
    )
    return (
        attn_out[None],
        grad_aq.astype(F32).T,
        grad_bq.astype(F32),
        grad_av.astype(F32).T,
        grad_bv.astype(F32),
    )


def solution(mesh):
    return jax.shard_map(
        on_device,
        mesh=mesh,
        in_specs=(
            P(None, None, "gx"),
            P("gy", None, "gx"),
            P("gx", "gy"),
            P("gx", "gy"),
            P("gy", "gx"),
            P("gx", None),
            P("gy", "gx", None),
            P(),
            P(None, "gy"),
            P(None, "gy"),
            P(None, "gy"),
            P(),
            P(),
            P(),
            P(),
            P("gy", "gx"),
            P("gy"),
            P("gy", "gx", None),
        ),
        out_specs=(P("gy", "gx", None), P(), P(), P(), P()),
        check_vma=False,
    )
```
